128 devices in a mesh: seq: 16 (over z, y), head: 8 (over x, core).
Axes of the slice: x: 4, y: 4, z: 4, core: 2. Of those that a mesh axis runs over, the one named last changes fastest.
Arguments:
- prompt_tokens: bfloat16 [2, 4096, 8192], P(None, ('seq', 'head')), may hold values from -6 to 6
- prompt_write: bfloat16 [2, 4096, 1024], P(None, 'seq', 'head'), may hold values from -0.47851562 to 0.47851562
- prompt_read: bfloat16 [2, 4096, 1024], P(None, 'seq', 'head'), may hold values from -0.47851562 to 0.47851562
- prompt_decay: float32 [2, 128, 4096], P(None, 'head', 'seq'), may hold values from -1 to 0, as said below
- prompt_cotangent: bfloat16 [2, 4096, 8192], P(None, 'seq', 'head'), may hold values from -6 to 6
- answer_tokens: bfloat16 [16, 256, 8192], P('seq', 'head'), may hold values from -6 to 6
- answer_write: bfloat16 [16, 256, 1024], P('seq', None, 'head'), may hold values from -0.47851562 to 0.47851562
- answer_read: bfloat16 [16, 256, 1024], P('seq', None, 'head'), may hold values from -0.47851562 to 0.47851562
- answer_decay: float32 [16, 128, 256], P('seq', 'head'), may hold values from -1 to 0, as said below
- answer_cotangent: bfloat16 [16, 256, 8192], P('seq', None, 'head'), may hold values from -6 to 6
- group_sizes: int32 [2], replicated, may hold values from 4 to 12, as said below
- answer_lengths: int32 [16], P('seq'), may hold values from 1 to 256, 2560 in all
Outputs:
- prompt_output: bfloat16 [2, 4096, 8192], P(None, 'seq', 'head')
- prompt_tokens_adjoint: bfloat16 [2, 4096, 8192], P(None, ('seq', 'head'))
- prompt_write_adjoint: bfloat16 [2, 4096, 1024], P(None, 'seq', 'head')
- prompt_read_adjoint: bfloat16 [2, 4096, 1024], P(None, 'seq', 'head')
- prompt_decay_adjoint: float32 [2, 128, 4096], P(None, 'head', 'seq')
- answer_output: bfloat16 [16, 256, 8192], P('seq', None, 'head')
- answer_tokens_adjoint: bfloat16 [16, 256, 8192], P('seq', 'head')
- answer_write_adjoint: bfloat16 [16, 256, 1024], P('seq', None, 'head')
- answer_read_adjoint: bfloat16 [16, 256, 1024], P('seq', None, 'head')
- answer_decay_adjoint: float32 [16, 128, 256], P('seq', 'head')
The draws below stay inside these ranges and needn't reach their ends.
Inputs may be any that keep to these rules, and one draw needn't show every extreme that they name: Completions are stored in prompt order: the first group_sizes[0] completions follow prompt 0, the next group_sizes[1] prompt 1, and so on; the sizes sum to 16, and one prompt has exactly 12. Completion i has loss and outputs at its first answer_lengths[i] positions only. `prompt_decay`: log decays are negative. `answer_decay`: log decays are negative.
All inputs are finite; a program needn't handle non-finite values. No bound on the sum of `answer_lengths` on one device may be relied on, other than what follows from the above.
Results may differ from the reference program's by a relative error of at most 0.015.
Values may be sent and summed in bfloat16 or wider, within the bound.
No kernel may reach another device: no remote copies, remote signals or barrier semaphores. Data moves between devices by JAX's collectives and lax.ppermute only.
A program may use at most 128 MiB of HBM per device.

```python
import math
from functools import partial
import jax
import jax.numpy as jnp
import numpy as np
from jax import lax

HEADS = 128
HEAD_DIM = 64
STATE = 128
GROUPS = 8
BLOCK = 256
PROMPTS = 2
PCH = 256
CLEN = 256
PLEN = 4096
ANSWERS = 16


def decay_law(key, count_of_rows, head_count, total_length, horizon, segment):
    random_subkeys = jax.random.split(key, 7)
    fast_share = 0.5
    fast_heads = jax.random.uniform(random_subkeys[0], (count_of_rows, head_count)) < fast_share
    slow_rate = jnp.exp(jax.random.uniform(random_subkeys[1], (count_of_rows, head_count), minval=jnp.log(0.05), maxval=jnp.log(0.6))) / horizon
    fast_rate = jnp.exp(jax.random.uniform(random_subkeys[2], (count_of_rows, head_count), minval=jnp.log(1.0 / 50.0), maxval=jnp.log(1.0 / 30.0)))
    decay_speed = jnp.where(fast_heads, fast_rate, slow_rate)
    jaggedness = jax.random.uniform(random_subkeys[3], (count_of_rows, head_count, total_length), minval=0.5, maxval=1.5)
    local_region = jnp.exp(jax.random.uniform(random_subkeys[4], (count_of_rows, head_count, total_length // segment), minval=jnp.log(0.7), maxval=jnp.log(1.4)))
    local_region = jnp.repeat(local_region, segment, axis=2)
    spike_events = jax.random.uniform(random_subkeys[5], (count_of_rows, total_length)) < 3.0 / total_length
    magnitude = jax.random.uniform(random_subkeys[6], (count_of_rows, head_count, total_length), minval=0.22, maxval=0.69)
    return -(decay_speed[..., None] * jaggedness * local_region + jnp.where(spike_events[:, None, :], magnitude, 0.0))


def draw_prompt_decay(key, part):
    return decay_law(jax.random.fold_in(key, 11), PROMPTS, HEADS, PLEN, PLEN, PCH).astype(jnp.float32)


def draw_answer_decay(key, part):
    return decay_law(jax.random.fold_in(key, 23), ANSWERS, HEADS, CLEN, CLEN, BLOCK).astype(jnp.float32)


def draw_group_sizes(key, part):
    larger = 3 * ANSWERS // 4
    smaller = ANSWERS - larger
    flipped = jax.random.randint(jax.random.fold_in(key, 37), (), 0, 2)
    first = jnp.where(flipped == 0, larger, smaller)
    second = jnp.where(flipped == 0, smaller, larger)
    return jnp.stack([first, second]).astype(jnp.int32)


def block_levels(key, extent, pieces, low, largest):
    loudness, own = 1.0, jax.random.fold_in(key, 6)
    for position, blocks in pieces:
        steps = jnp.exp(jax.random.uniform(jax.random.fold_in(own, position), (blocks,), jnp.float32, low / len(pieces), largest / len(pieces)))
        loudness = loudness * jnp.repeat(steps, extent[position] // blocks).reshape([-1 if axis == position else 1 for axis in range(len(extent))])
    return loudness


def length_profile(count, total, bound, skew):
    loads = [(1 << 20) // math.isqrt(grade ** skew) + 1 for grade in range(2, count + 1)]
    spare, holding = total - bound - (count - 1), [1] * (count - 1)
    while spare > 0:
        candidates = [i for i in range(count - 1) if holding[i] < bound]
        mass, left = sum([loads[i] for i in candidates]), spare
        for i in candidates:
            more = min(bound - holding[i], max(1, left * loads[i] // mass), spare)
            holding[i] = holding[i] + more
            spare = spare - more
    return np.array([bound] + holding)


def ragged_sizes(rng, count, total, most, lean):
    if count == 2:
        one = jax.random.randint(rng, (), max(1, total - most), min(most, total - 1) + 1)
        return jnp.stack([one, total - one])
    sizes = jnp.asarray(length_profile(count, total, most, lean), jnp.int32)
    twos = (count - 1) // 2
    source_of, receiver = sizes[1:1 + 2 * twos:2], sizes[2:2 + 2 * twos:2]
    slack = jnp.minimum(source_of - 1, most - receiver)
    moved = jax.random.randint(jax.random.fold_in(rng, 1), (twos,), 0, 1 << 20) % (slack + 1)
    sizes = sizes.at[1:1 + 2 * twos:2].set(source_of - moved).at[2:2 + 2 * twos:2].set(receiver + moved)
    return sizes[jax.random.permutation(jax.random.fold_in(rng, 2), count)]


def centred(stream_key, dims, width, reach, pieces=(), kind=jnp.bfloat16):
    array = width * jax.random.normal(stream_key, dims, jnp.float32)
    if pieces:
        array = array * block_levels(stream_key, dims, pieces, -0.22, 0.18)
    return jnp.clip(array, -reach, reach).astype(kind)


def setup_inputs(seed: int = 0) -> dict:
    keys = jax.random.split(jax.random.key(seed), 13)
    prompt_tokens = centred(keys[0], (PROMPTS, PLEN, HEADS * HEAD_DIM), 1.0, 6.0, ((1, 128),))
    prompt_write = centred(keys[1], (PROMPTS, PLEN, GROUPS * STATE), 0.08, 0.47851562, ((1, 16), (2, 8)))
    prompt_read = centred(keys[2], (PROMPTS, PLEN, GROUPS * STATE), 0.08, 0.47851562, ((1, 16), (2, 8)))
    prompt_decay = draw_prompt_decay(jax.random.fold_in(keys[12], 71), 0)
    prompt_cotangent = centred(keys[4], (PROMPTS, PLEN, HEADS * HEAD_DIM), 1.0, 6.0, ((1, 16), (2, 8)))
    answer_tokens = centred(keys[5], (ANSWERS, CLEN, HEADS * HEAD_DIM), 1.0, 6.0, ((0, 16), (1, 8)))
    answer_write = centred(keys[6], (ANSWERS, CLEN, GROUPS * STATE), 0.08, 0.47851562, ((0, 16), (2, 8)))
    answer_read = centred(keys[7], (ANSWERS, CLEN, GROUPS * STATE), 0.08, 0.47851562, ((0, 16), (2, 8)))
    answer_decay = draw_answer_decay(jax.random.fold_in(keys[12], 71), 0)
    answer_cotangent = centred(keys[9], (ANSWERS, CLEN, HEADS * HEAD_DIM), 1.0, 6.0, ((0, 16), (2, 8)))
    group_sizes = draw_group_sizes(jax.random.fold_in(keys[12], 71), 0)
    answer_lengths = ragged_sizes(keys[11], ANSWERS, ANSWERS * CLEN * 5 // 8, CLEN, 1).astype(jnp.int32)
    return {"prompt_tokens": prompt_tokens, "prompt_write": prompt_write, "prompt_read": prompt_read, "prompt_decay": prompt_decay, "prompt_cotangent": prompt_cotangent, "answer_tokens": answer_tokens, "answer_write": answer_write, "answer_read": answer_read, "answer_decay": answer_decay, "answer_cotangent": answer_cotangent, "group_sizes": group_sizes, "answer_lengths": answer_lengths}


def contract(pattern, first_operand, second_operand):
    return jnp.einsum(pattern, first_operand.astype(jnp.float32), second_operand.astype(jnp.float32), precision=lax.Precision.HIGHEST)

def ssd_scan(tokens, key_inputs, query_inputs, log_decay, initial, block_size):
    total_length = tokens.shape[0]
    head_count, state_size, head_size = initial.shape
    groups = key_inputs.shape[1] // state_size
    per_group = head_count // groups
    blocks = total_length // block_size
    values = tokens.reshape(blocks, block_size, groups, per_group, head_size)
    key_rows = key_inputs.reshape(blocks, block_size, groups, state_size)
    queries = query_inputs.reshape(blocks, block_size, groups, state_size)
    running = jnp.cumsum(log_decay.reshape(groups, per_group, blocks, block_size).transpose(2, 0, 1, 3), axis=3)
    closing = running[..., -1]
    scores = contract('cign,cjgn->cgij', queries, key_rows)
    causal = lax.broadcasted_iota(jnp.int32, (block_size, block_size), 0) >= lax.broadcasted_iota(jnp.int32, (block_size, block_size), 1)
    spread = running[..., :, None] - running[..., None, :]
    weights = jnp.where(causal, jnp.exp(jnp.where(causal, spread, 0.0)), 0.0)
    mixing = (weights * scores[:, :, None]).astype(jnp.bfloat16)
    inside = contract('cghij,cjghp->cighp', mixing, values)
    to_close = jnp.exp(closing[..., None] - running).transpose(0, 3, 1, 2)
    weighted = (values.astype(jnp.float32) * to_close[..., None]).astype(jnp.bfloat16)
    block_states = contract('cjgn,cjghp->cghnp', key_rows, weighted)

    def advance(carried, scan_item):
        fresh_state, factor = scan_item
        return (jnp.exp(factor)[..., None, None] * carried + fresh_state, carried)
    ending, starting = lax.scan(advance, initial.reshape(groups, per_group, state_size, head_size), (block_states, closing))
    outside = contract('cign,cghnp->cighp', queries, starting.astype(jnp.bfloat16))
    outside = outside * jnp.exp(running).transpose(0, 3, 1, 2)[..., None]
    output = (inside + outside).reshape(total_length, head_count * head_size)
    return (output, ending.reshape(head_count, state_size, head_size))

def regroup_columns(stacked):
    shape = stacked.shape
    return stacked.transpose(1, 2, 0, 3).reshape(shape[1], shape[2], shape[0] * shape[3])

def regroup_rows(stacked):
    shape = stacked.shape
    return stacked.transpose(1, 0, 2, 3).reshape(shape[1], shape[0] * shape[2], shape[3])

def reference(prompt_tokens, prompt_write, prompt_read, prompt_decay, prompt_cotangent, answer_tokens, answer_write, answer_read, answer_decay, answer_cotangent, group_sizes, answer_lengths):
    per_group = HEADS // GROUPS
    slots = jnp.arange(ANSWERS, dtype=jnp.int32)
    bounds = jnp.cumsum(group_sizes).astype(jnp.int32)
    owner = lax.optimization_barrier(jnp.sum((slots[:, None] >= bounds[None, :]).astype(jnp.int32), axis=1))
    live = jnp.arange(CLEN, dtype=jnp.int32)[None, :] < answer_lengths[:, None]
    answer_seed = jnp.where(live[..., None], answer_cotangent, jnp.zeros_like(answer_cotangent)).astype(jnp.float32)
    prompt_seed = prompt_cotangent.astype(jnp.float32)
    batched = jax.vmap(partial(ssd_scan, block_size=BLOCK))

    def one_group(group_index):
        column = group_index * (per_group * HEAD_DIM)
        state_column = group_index * STATE
        head_row = group_index * per_group
        p_tok = lax.dynamic_slice_in_dim(prompt_tokens, column, per_group * HEAD_DIM, 2)
        p_wri = lax.dynamic_slice_in_dim(prompt_write, state_column, STATE, 2)
        p_rea = lax.dynamic_slice_in_dim(prompt_read, state_column, STATE, 2)
        p_dec = lax.dynamic_slice_in_dim(prompt_decay, head_row, per_group, 1)
        a_tok = lax.dynamic_slice_in_dim(answer_tokens, column, per_group * HEAD_DIM, 2)
        a_wri = lax.dynamic_slice_in_dim(answer_write, state_column, STATE, 2)
        a_rea = lax.dynamic_slice_in_dim(answer_read, state_column, STATE, 2)
        a_dec = lax.dynamic_slice_in_dim(answer_decay, head_row, per_group, 1)

        def forward(tok_one, wri_one, rea_one, dec_one, tok_two, wri_two, rea_two, dec_two):
            blank = jnp.zeros((PROMPTS, per_group, STATE, HEAD_DIM), jnp.float32)
            prompt_result, prompt_end = batched(tok_one, wri_one, rea_one, dec_one, blank)
            answer_start = prompt_end[owner]
            answer_result = batched(tok_two, wri_two, rea_two, dec_two, answer_start)[0]
            return (prompt_result, answer_result)
        results, pull = jax.vjp(forward, p_tok, p_wri, p_rea, p_dec, a_tok, a_wri, a_rea, a_dec)
        seeds = (lax.dynamic_slice_in_dim(prompt_seed, column, per_group * HEAD_DIM, 2), lax.dynamic_slice_in_dim(answer_seed, column, per_group * HEAD_DIM, 2))
        grads = pull(seeds)
        answer_out = jnp.where(live[..., None], results[1], 0.0).astype(jnp.bfloat16)
        return (results[0].astype(jnp.bfloat16), grads[0], grads[1], grads[2], grads[3], answer_out, grads[4], grads[5], grads[6], grads[7])
    stacked = lax.map(one_group, jnp.arange(GROUPS, dtype=jnp.int32))
    return (regroup_columns(stacked[0]), regroup_columns(stacked[1]), regroup_columns(stacked[2]), regroup_columns(stacked[3]), regroup_rows(stacked[4]), regroup_columns(stacked[5]), regroup_columns(stacked[6]), regroup_columns(stacked[7]), regroup_columns(stacked[8]), regroup_rows(stacked[9]))
```

```python
import jax
import jax.numpy as jnp
from jax import lax
from jax.experimental import pallas as pl
from jax.experimental.pallas import tpu as pltpu
from jax.sharding import PartitionSpec as P


HD = 64
N = 128
B = 256
H = 16
L = H * HD
SHARDS = 16
GROUP = 8
ROWS = B // GROUP
HALF = L // 2
F32 = jnp.float32
BF16 = jnp.bfloat16


def nn(a, b):
    return lax.dot_general(a, b, (((1,), (0,)), ((), ())), preferred_element_type=F32)


def nt(a, b):
    return lax.dot_general(a, b, (((1,), (1,)), ((), ())), preferred_element_type=F32)


def tn(a, b):
    return lax.dot_general(a, b, (((0,), (0,)), ((), ())), preferred_element_type=F32)


def iota(shape, axis):
    return lax.broadcasted_iota(jnp.int32, shape, axis)


def terms(value):
    high = value.astype(BF16)
    rest = value - high.astype(F32)
    middle = rest.astype(BF16)
    return high, middle, (rest - middle.astype(F32)).astype(BF16)


def upper():
    return (iota((B, B), 0) <= iota((B, B), 1)).astype(BF16)


def lower():
    return (iota((B, B), 1) <= iota((B, B), 0)).astype(BF16)


def running_rows(decay):
    parts = nn(jnp.concatenate([part.astype(F32) for part in terms(decay)], axis=0).astype(BF16), upper())
    return parts[:H] + parts[H : 2 * H] + parts[2 * H :]


def running_columns(decay):
    tri = lower()
    total = None
    for part in terms(decay):
        wide = part.astype(F32)
        added = nt(tri, jnp.concatenate([wide, wide, wide], axis=0).astype(BF16))
        total = added if total is None else total + added
    return total


def widened(columns):
    lane = iota(columns.shape, 1)
    high = columns.astype(BF16).astype(F32)
    rest = columns - high
    middle = rest.astype(BF16).astype(F32)
    packed = jnp.where(lane < H, high, jnp.where(lane < 2 * H, middle, rest - middle)).astype(BF16)
    member = (iota((3 * H, L), 1) // HD == iota((3 * H, L), 0) % H).astype(BF16)
    return nn(packed, member)


def grown(decay):
    return widened(jnp.exp(running_columns(decay)))


def closing_weight(decay):
    columns = running_columns(decay)
    return widened(jnp.exp(columns[B - 1 : B, :] - columns))


def head_sums(values):
    member = (iota((L, H), 0) // HD == iota((L, H), 1)).astype(BF16)
    high = values.astype(BF16)
    low = (values - high.astype(F32)).astype(BF16)
    return nn(high, member) + nn(low, member)


def live_rows(value, length):
    return jnp.where(iota(value.shape, 0) < length, value, jnp.zeros_like(value))


def piece(d):
    return slice(16 * (d // 2), 16 * (d // 2) + 16), slice(HALF * (d % 2), HALF * (d % 2) + HALF)


def scattered(out, state, first):
    for d in range(SHARDS):
        rows, lanes = piece(d)
        out[16 * d : 16 * d + 16, first : first + HALF] = state[rows, lanes].astype(BF16)


def gathered(m, place):
    for d in range(SHARDS):
        rows, lanes = piece(d)
        place[rows, lanes] = m[16 * d : 16 * d + 16, :]


def assembled(me, chunks, x):
    for k in range(GROUP):
        there = pl.multiple_of((me[0] ^ k) * ROWS, ROWS)
        x[pl.ds(there, ROWS), :] = chunks[k][0]


def reach_kernel(length, pr, pd, pc, ar, ad, ac, out, factors):
    b = pl.program_id(0)

    @pl.when(b < 3)
    def _():
        answer = b == 2
        read = jnp.where(answer, ar[0], pr[0])
        decay = jnp.where(answer, ad[0], pd[0])
        alive = jnp.where(answer, length[0], B)
        cot = live_rows(jnp.where(answer, ac[0], pc[0]).astype(F32), alive)
        growth = grown(decay)
        scattered(out, tn(read, (cot * growth).astype(BF16)), 0)
        last = growth[B - 1 : B, :]
        high = last.astype(BF16).astype(F32)
        row = iota((16, L), 0) - 2 * b
        part = jnp.where(row == 0, high, jnp.where(row == 1, last - high, 0.0))
        factors[...] = jnp.where(b == 0, part, jnp.where(answer, factors[...], factors[...] + part))

    @pl.when(b == 3)
    def _():
        for d in range(SHARDS):
            out[16 * d : 16 * d + 16, :] = factors[:, piece(d)[1]].astype(BF16)


def split_kernel(me, pt, at, *outs):
    b = pl.program_id(0)
    for k in range(GROUP):
        there = pl.multiple_of((me[0] ^ k) * L, L)
        outs[k][0] = jnp.where(b == 2, at[0, :, pl.ds(there, L)], pt[0, :, pl.ds(there, L)])


def join_kernel(me, *refs):
    b = pl.program_id(0)
    ins, (pt, at) = refs[:GROUP], refs[GROUP:]
    for k in range(GROUP):
        there = pl.multiple_of((me[0] ^ k) * L, L)

        @pl.when(b < 2)
        def _():
            pt[0, :, pl.ds(there, L)] = ins[k][0]

        @pl.when(b == 2)
        def _():
            at[0, :, pl.ds(there, L)] = ins[k][0]


def shard_factor(factors, k, q):
    part = factors[16 * k : 16 * k + 16, :].astype(F32)
    row = iota((16, HALF), 0) - 2 * q
    return jnp.sum(jnp.where((row == 0) | (row == 1), part, 0.0), axis=0, keepdims=True)


def owner_of(sizes, k):
    return (sizes[0] <= k).astype(jnp.int32) + (sizes[0] + sizes[1] <= k).astype(jnp.int32)


def close_kernel(me, sizes, reach, answers, factors, pw, pd, *refs):
    q = pl.program_id(0)
    chunks, (out, x) = refs[:GROUP], refs[GROUP:]
    assembled(me, chunks, x)
    weighted = (x[...].astype(F32) * closing_weight(pd[0])).astype(BF16)
    scattered(out, tn(pw[0], weighted), HALF)
    grad = jnp.zeros((16, HALF), F32)
    for k in range(SHARDS):
        part = answers[16 * k : 16 * k + 16, :].astype(F32)
        grad = grad + part * (owner_of(sizes, k) == q).astype(F32)
    for k in reversed(range(SHARDS)):
        out[16 * k : 16 * k + 16, :HALF] = grad.astype(BF16)
        grad = reach[16 * k : 16 * k + 16, :].astype(F32) + shard_factor(factors, k, q) * grad


def start_kernel(sizes, factors, first, second, out):
    ends = []
    for q, local in enumerate((first, second)):
        state = jnp.zeros((16, HALF), F32)
        for k in range(SHARDS):
            out[16 * k : 16 * k + 16, q * HALF : (q + 1) * HALF] = state.astype(BF16)
            state = shard_factor(factors, k, q) * state + local[16 * k : 16 * k + 16, :].astype(F32)
        ends.append(state)
    for k in range(SHARDS):
        owner = owner_of(sizes, k)
        mine = ends[0] * (owner == 0).astype(F32) + ends[1] * (owner == 1).astype(F32)
        out[16 * k : 16 * k + 16, 2 * HALF : 3 * HALF] = mine.astype(BF16)


def inside_kernel(length, me, pw, pr, pd, pc, aw, ar, ad, ac, *refs):
    chunks, (y_out, dx_out, dr_out, dw_out, adw, z_out, x, zs) = refs[:GROUP], refs[GROUP:]
    b = pl.program_id(0)
    answer = b == 2
    write = jnp.where(answer, aw[0], pw[0])
    read = jnp.where(answer, ar[0], pr[0])
    decay = jnp.where(answer, ad[0], pd[0])
    alive = jnp.where(answer, length[0], B)
    cot32 = live_rows(jnp.where(answer, ac[0], pc[0]).astype(F32), alive)
    cot_t = cot32.T.astype(BF16)
    assembled(me, chunks, x)
    rows = running_rows(decay)
    columns = running_columns(decay)
    scores = nt(read, write)
    causal = iota((B, B), 0) >= iota((B, B), 1)
    first = iota((B, 2 * HD), 1) < HD
    grad = jnp.zeros((B, B), F32)
    for pair in range(H // 2):
        lanes = slice(2 * HD * pair, 2 * HD * pair + 2 * HD)
        xs = x[:, lanes]
        cs = cot32[:, lanes]
        ys, dxs = [], []
        for s in range(2):
            h = 2 * pair + s
            gap = columns[:, h : h + 1] - rows[h : h + 1, :]
            weight = jnp.exp(jnp.where(causal, gap, -1e30))
            mixing = (weight * scores).astype(BF16)
            ys.append(nn(mixing, xs))
            dxs.append(nn(cot_t[HD * h : HD * h + HD, :], mixing))
            own = jnp.where(first if s == 0 else jnp.logical_not(first), cs, 0.0).astype(BF16)
            grad = grad + nt(own, xs) * weight
        y = jnp.where(first, ys[0], ys[1])
        dx = jnp.concatenate(dxs, axis=0).T
        y_out[0, :, lanes] = y.astype(BF16)
        dx_out[0, :, lanes] = dx.astype(BF16)
        zs[:, lanes] = cs * y - xs.astype(F32) * dx
    z_out[0] = head_sums(zs[...])
    grad = grad.astype(BF16)
    dr_out[0] = nn(grad, write)
    dw = tn(grad, read)

    @pl.when(b < 2)
    def _():
        dw_out[0] = dw

    @pl.when(answer)
    def _():
        adw[0] = dw.astype(BF16)


def token_kernel(me, m2, pw, pd, dxi, *refs):
    outs, (ends, full) = refs[:GROUP], refs[GROUP:]
    b = pl.program_id(0)

    @pl.when(b < 2)
    def _():
        gathered(m2, ends)
        full[...] = (dxi[0].astype(F32) + nn(pw[0], ends[...]) * closing_weight(pd[0])).astype(BF16)

    @pl.when(b == 2)
    def _():
        full[...] = dxi[0]

    for k in range(GROUP):
        there = pl.multiple_of((me[0] ^ k) * ROWS, ROWS)
        outs[k][0] = full[pl.ds(there, ROWS), :]


def write_kernel(me, m2, pw, pd, dwi, *refs):
    chunks, (pdw, z, closing, x, ends) = refs[:GROUP], refs[GROUP:]
    assembled(me, chunks, x)
    gathered(m2, ends)
    xs = x[...].astype(F32)
    to_close = closing_weight(pd[0])
    weighted = (xs * to_close).astype(BF16)
    pdw[0] = (dwi[0] + nt(weighted, ends[...])).astype(BF16)
    tail = xs * (nn(pw[0], ends[...]) * to_close)
    closing[0] = jnp.broadcast_to(jnp.sum(tail, axis=0, keepdims=True), (8, L))
    z[0] = head_sums(tail)


def output_kernel(
    length, m2, m3, pr, pd, pc, ar, ad, ac, yi, dri, zi, z, closing, py, pdr, pdd, ay, adr, add, start, ends
):
    b = pl.program_id(0)
    answer = b == 2
    gathered(m3, start)
    read = jnp.where(answer, ar[0], pr[0])
    decay = jnp.where(answer, ad[0], pd[0])
    alive = jnp.where(answer, length[0], B)
    cot = live_rows(jnp.where(answer, ac[0], pc[0]).astype(F32), alive)
    growth = grown(decay)
    outside = nn(read, start[...]) * growth
    y = yi[0].astype(F32) + outside
    dr = dri[0] + nt((cot * growth).astype(BF16), start[...])
    zs = zi[0] + head_sums(cot * outside) - jnp.where(answer, 0.0, z[0])
    tri = lower()
    dd = sum(tn(part, tri) for part in terms(zs))

    @pl.when(b < 2)
    def _():
        gathered(m2, ends)
        inner = jnp.sum(ends[...].astype(F32) * start[...].astype(F32), axis=0, keepdims=True)
        last = closing[0] + inner * growth[B - 1 : B, :]
        member = (iota((H, L), 1) // HD == iota((H, L), 0)).astype(BF16)
        total = sum(nt(member, part) for part in terms(last))
        py[0] = y.astype(BF16)
        pdr[0] = dr.astype(BF16)
        pdd[0] = dd + total[:, 0:1]

    @pl.when(answer)
    def _():
        ay[0] = live_rows(y, length[0]).astype(BF16)
        adr[0] = dr.astype(BF16)
        add[0] = dd


SMEM = pl.BlockSpec(memory_space=pltpu.SMEM)


def own(*dims):
    return pl.BlockSpec((1, *dims), lambda b: (jnp.minimum(b, 1), 0, 0))


def one(*dims):
    return pl.BlockSpec((1, *dims), lambda b: (0, 0, 0))


def each(*dims):
    return pl.BlockSpec((1, *dims), lambda b: (b, 0, 0))


def column(width, index):
    return pl.BlockSpec((B, width), lambda b: (0, index(b)))


def shape(dims, dtype=BF16):
    return jax.ShapeDtypeStruct(dims, dtype)


def call(kernel, steps, ins, outs, args, scratch=(), flops=1e9):
    return pl.pallas_call(
        kernel,
        grid=(steps,),
        in_specs=ins,
        out_specs=[spec for spec, _ in outs],
        out_shape=[struct for _, struct in outs],
        scratch_shapes=scratch,
        cost_estimate=pl.CostEstimate(flops=int(flops), bytes_accessed=4000000, transcendentals=0),
    )(*args)


def exchange(chunks):
    sent = [chunks[0]]
    for k in range(1, GROUP):
        sent.append(lax.ppermute(chunks[k], "head", [(i, i ^ k) for i in range(GROUP)]))
    return sent


def transposed(message):
    return lax.all_to_all(message, "seq", split_axis=0, concat_axis=0, tiled=True)


def per_device(pt, pw, pr, pd, pc, at, aw, ar, ad, ac, sizes, length):
    me = lax.axis_index("head").astype(jnp.int32).reshape(1)
    state = pltpu.VMEM((N, L), BF16)
    block = pltpu.VMEM((B, L), BF16)
    chunk = [(each(ROWS, L), shape((3, ROWS, L))) for _ in range(GROUP)]
    pieces = [each(ROWS, L)] * GROUP
    prompt_side = [own(B, N), own(H, B), own(B, L)]
    answer_side = [one(B, N), one(H, B), one(B, L)]
    (m1,) = call(
        reach_kernel,
        4,
        [SMEM, *prompt_side, *answer_side],
        [(column(HALF, lambda b: b), shape((B, 4 * HALF)))],
        (length, pr, pd, pc, ar, ad, ac),
        (pltpu.VMEM((16, L), F32),),
    )
    m1 = transposed(m1)
    cut = call(split_kernel, 3, [SMEM, own(ROWS, GROUP * L), one(ROWS, GROUP * L)], chunk, (me, pt, at))
    cut = exchange(cut)
    (m2,) = call(
        close_kernel,
        2,
        [
            SMEM,
            SMEM,
            column(HALF, lambda q: q),
            column(HALF, lambda q: 2),
            column(HALF, lambda q: 3),
            each(B, N),
            each(H, B),
            *pieces,
        ],
        [(column(2 * HALF, lambda q: q), shape((B, 4 * HALF)))],
        (me, sizes, m1, m1, m1, pw, pd, *cut),
        (block,),
    )
    m2 = transposed(m2)
    yi, dxi, dri, dwi, adw, zi = call(
        inside_kernel,
        3,
        [SMEM, SMEM, own(B, N), *prompt_side, one(B, N), *answer_side, *pieces],
        [
            (each(B, L), shape((3, B, L))),
            (each(B, L), shape((3, B, L))),
            (each(B, N), shape((3, B, N), F32)),
            (own(B, N), shape((2, B, N), F32)),
            (one(B, N), shape((1, B, N))),
            (each(B, H), shape((3, B, H), F32)),
        ],
        (length, me, pw, pr, pd, pc, aw, ar, ad, ac, *cut),
        (block, pltpu.VMEM((B, L), F32)),
        8e9,
    )
    (m3,) = call(
        start_kernel,
        1,
        [SMEM, column(HALF, lambda b: 3), column(HALF, lambda b: 1), column(HALF, lambda b: 3)],
        [(column(3 * HALF, lambda b: 0), shape((B, 3 * HALF)))],
        (sizes, m1, m2, m2),
    )
    m3 = transposed(m3)
    back = call(
        token_kernel,
        3,
        [SMEM, column(HALF, lambda b: 2 * jnp.minimum(b, 1)), own(B, N), own(H, B), each(B, L)],
        chunk,
        (me, m2, pw, pd, dxi),
        (state, block),
    )
    back = exchange(back)
    pdw, z, closing = call(
        write_kernel,
        2,
        [SMEM, column(HALF, lambda q: 2 * q), each(B, N), each(H, B), each(B, N), *pieces],
        [
            (each(B, N), shape((2, B, N))),
            (each(B, H), shape((2, B, H), F32)),
            (each(8, L), shape((2, 8, L), F32)),
        ],
        (me, m2, pw, pd, dwi, *cut),
        (block, state),
    )
    py, pdr, pdd, ay, adr, add = call(
        output_kernel,
        3,
        [
            SMEM,
            column(HALF, lambda b: 2 * jnp.minimum(b, 1)),
            column(HALF, lambda b: b),
            *prompt_side,
            *answer_side,
            each(B, L),
            each(B, N),
            each(B, H),
            own(B, H),
            own(8, L),
        ],
        [
            (own(B, L), shape((2, B, L))),
            (own(B, N), shape((2, B, N))),
            (own(H, B), shape((2, H, B), F32)),
            (one(B, L), shape((1, B, L))),
            (one(B, N), shape((1, B, N))),
            (one(H, B), shape((1, H, B), F32)),
        ],
        (length, m2, m3, pr, pd, pc, ar, ad, ac, yi, dri, zi, z, closing),
        (state, state),
    )
    pdx, adx = call(
        join_kernel,
        3,
        [SMEM, *pieces],
        [
            (own(ROWS, GROUP * L), shape((2, ROWS, GROUP * L))),
            (one(ROWS, GROUP * L), shape((1, ROWS, GROUP * L))),
        ],
        (me, *back),
    )
    return py, pdx, pdw, pdr, pdd, ay, adx, adw, adr, add


def solution(mesh):
    split_positions = P(None, ("seq", "head"), None)
    prompt = P(None, "seq", "head")
    answer = P("seq", None, "head")
    return jax.shard_map(
        per_device,
        mesh=mesh,
        in_specs=(
            split_positions,
            prompt,
            prompt,
            P(None, "head", "seq"),
            prompt,
            P("seq", "head", None),
            answer,
            answer,
            P("seq", "head", None),
            answer,
            P(),
            P("seq"),
        ),
        out_specs=(
            prompt,
            split_positions,
            prompt,
            prompt,
            P(None, "head", "seq"),
            answer,
            P("seq", "head", None),
            answer,
            answer,
            P("seq", "head", None),
        ),
        check_vma=False,
    )
```

```python
import jax
import jax.numpy as jnp
from jax import lax
from jax.experimental import pallas as pl
from jax.experimental.pallas import tpu as pltpu
from jax.sharding import PartitionSpec as P


HD = 64
N = 128
B = 256
H = 16
L = H * HD
SHARDS = 16
GROUP = 8
ROWS = B // GROUP
HALF = L // 2
F32 = jnp.float32
BF16 = jnp.bfloat16


def nn(a, b):
    return lax.dot_general(a, b, (((1,), (0,)), ((), ())), preferred_element_type=F32)


def nt(a, b):
    return lax.dot_general(a, b, (((1,), (1,)), ((), ())), preferred_element_type=F32)


def tn(a, b):
    return lax.dot_general(a, b, (((0,), (0,)), ((), ())), preferred_element_type=F32)


def iota(shape, axis):
    return lax.broadcasted_iota(jnp.int32, shape, axis)


def terms(value):
    high = value.astype(BF16)
    rest = value - high.astype(F32)
    middle = rest.astype(BF16)
    return high, middle, (rest - middle.astype(F32)).astype(BF16)


def upper():
    return (iota((B, B), 0) <= iota((B, B), 1)).astype(BF16)


def lower():
    return (iota((B, B), 1) <= iota((B, B), 0)).astype(BF16)


def running_rows(decay):
    parts = nn(jnp.concatenate([part.astype(F32) for part in terms(decay)], axis=0).astype(BF16), upper())
    return parts[:H] + parts[H : 2 * H] + parts[2 * H :]


def running_columns(decay):
    tri = lower()
    total = None
    for part in terms(decay):
        wide = part.astype(F32)
        added = nt(tri, jnp.concatenate([wide, wide, wide], axis=0).astype(BF16))
        total = added if total is None else total + added
    return total


def widened(columns):
    lane = iota(columns.shape, 1)
    high = columns.astype(BF16).astype(F32)
    rest = columns - high
    middle = rest.astype(BF16).astype(F32)
    packed = jnp.where(lane < H, high, jnp.where(lane < 2 * H, middle, rest - middle)).astype(BF16)
    member = (iota((3 * H, L), 1) // HD == iota((3 * H, L), 0) % H).astype(BF16)
    return nn(packed, member)


def grown(decay):
    return widened(jnp.exp(running_columns(decay)))


def closing_weight(decay):
    columns = running_columns(decay)
    return widened(jnp.exp(columns[B - 1 : B, :] - columns))


def head_sums(values):
    member = (iota((L, H), 0) // HD == iota((L, H), 1)).astype(BF16)
    high = values.astype(BF16)
    low = (values - high.astype(F32)).astype(BF16)
    return nn(high, member) + nn(low, member)


def live_rows(value, length):
    return jnp.where(iota(value.shape, 0) < length, value, jnp.zeros_like(value))


def piece(d):
    return slice(16 * (d // 2), 16 * (d // 2) + 16), slice(HALF * (d % 2), HALF * (d % 2) + HALF)


def scattered(out, state, first):
    for d in range(SHARDS):
        rows, lanes = piece(d)
        out[16 * d : 16 * d + 16, pl.ds(first, HALF)] = state[rows, lanes].astype(BF16)


def gathered(m, place):
    for d in range(SHARDS):
        rows, lanes = piece(d)
        place[rows, lanes] = m[16 * d : 16 * d + 16, :]


def assembled(me, chunks, x):
    for k in range(GROUP):
        there = pl.multiple_of((me[0] ^ k) * ROWS, ROWS)
        x[pl.ds(there, ROWS), :] = chunks[k][0]


def reach_kernel(length, pr, pd, pc, ar, ad, ac, out, factors):
    b = pl.program_id(0)
    answer = b == 2
    read = jnp.where(answer, ar[0], pr[0])
    decay = jnp.where(answer, ad[0], pd[0])
    alive = jnp.where(answer, length[0], B)
    cot = live_rows(jnp.where(answer, ac[0], pc[0]).astype(F32), alive)
    growth = grown(decay)
    scattered(out, tn(read, (cot * growth).astype(BF16)), pl.multiple_of(b * HALF, HALF))
    last = growth[B - 1 : B, :]
    high = last.astype(BF16).astype(F32)

    @pl.when(b < 2)
    def _():
        factors[pl.ds(2 * b, 1), :] = high
        factors[pl.ds(2 * b + 1, 1), :] = last - high

    @pl.when(answer)
    def _():
        for half in range(2):
            lanes = [slice(HALF * half + N * j, HALF * half + N * j + N) for j in range(4)]
            part = jnp.concatenate([factors[i : i + 1, lane] for i in range(4) for lane in lanes], axis=0)
            for d in range(half, SHARDS, 2):
                out[16 * d : 16 * d + 16, 3 * HALF :] = part.astype(BF16)


def split_kernel(me, pt, at, *refs):
    outs, (stage, came, went) = refs[:GROUP], refs[GROUP:]
    coming, going = [], []
    for k in (4, 5, 2, 3, 6, 7, 1, 0):
        there = pl.multiple_of((me[0] ^ k) * L, L)
        coming.append(
            (
                pltpu.make_async_copy(pt.at[:, :, pl.ds(there, L)], stage.at[k, 0:2], came.at[2 * k]),
                pltpu.make_async_copy(at.at[:, :, pl.ds(there, L)], stage.at[k, 2:3], came.at[2 * k + 1]),
            )
        )
        going.append(pltpu.make_async_copy(stage.at[k], outs[k], went.at[k]))
    for first, second in coming:
        first.start()
        second.start()
    for (first, second), third in zip(coming, going):
        first.wait()
        second.wait()
        third.start()
    for copy in going:
        copy.wait()


def join_kernel(me, *refs):
    ins, (pt, at, stage, came, went) = refs[:GROUP], refs[GROUP:]
    coming, going = [], []
    for k in range(GROUP):
        there = pl.multiple_of((me[0] ^ k) * L, L)
        coming.append(pltpu.make_async_copy(ins[k], stage.at[k], came.at[k]))
        going.append(
            (
                pltpu.make_async_copy(stage.at[k, 0:2], pt.at[:, :, pl.ds(there, L)], went.at[2 * k]),
                pltpu.make_async_copy(stage.at[k, 2:3], at.at[:, :, pl.ds(there, L)], went.at[2 * k + 1]),
            )
        )
    for copy in coming:
        copy.start()
    for first, (second, third) in zip(coming, going):
        first.wait()
        second.start()
        third.start()
    for second, third in going:
        second.wait()
        third.wait()


def shard_factor(packed, k, q):
    part = packed[16 * k : 16 * k + 16, :].astype(F32)
    rows = [part[8 * q + j : 8 * q + j + 1] + part[8 * q + 4 + j : 8 * q + 5 + j] for j in range(4)]
    return jnp.concatenate(rows, axis=1)


def owner_of(sizes, k):
    return (sizes[0] <= k).astype(jnp.int32) + (sizes[0] + sizes[1] <= k).astype(jnp.int32)


def local_kernel(me, message, pw, pd, *refs):
    chunks, (out, x) = refs[:GROUP], refs[GROUP:]
    assembled(me, chunks, x)
    weighted = (x[...].astype(F32) * closing_weight(pd[0])).astype(BF16)
    scattered(out, tn(pw[0], weighted), 0)


def turn_kernel(sizes, reach, answers, packed, out, factors):
    for q in range(2):
        grad = jnp.zeros((16, HALF), F32)
        for k in range(SHARDS):
            part = answers[16 * k : 16 * k + 16, :].astype(F32)
            grad = grad + part * (owner_of(sizes, k) == q).astype(F32)
        for k in reversed(range(SHARDS)):
            out[16 * k : 16 * k + 16, q * HALF : (q + 1) * HALF] = grad.astype(BF16)
            factor = shard_factor(packed, k, q)
            factors[16 * q + k : 16 * q + k + 1, :] = factor
            grad = reach[16 * k : 16 * k + 16, q * HALF : (q + 1) * HALF].astype(F32) + factor * grad


def start_kernel(sizes, factors, m2, out):
    ends = []
    for q in range(2):
        state = jnp.zeros((16, HALF), F32)
        for k in range(SHARDS):
            out[16 * k : 16 * k + 16, q * HALF : (q + 1) * HALF] = state.astype(BF16)
            local = m2[16 * k : 16 * k + 16, (2 + q) * HALF : (3 + q) * HALF].astype(F32)
            state = factors[16 * q + k : 16 * q + k + 1, :] * state + local
        ends.append(state)
    for k in range(SHARDS):
        owner = owner_of(sizes, k)
        mine = ends[0] * (owner == 0).astype(F32) + ends[1] * (owner == 1).astype(F32)
        out[16 * k : 16 * k + 16, 2 * HALF : 3 * HALF] = mine.astype(BF16)


def inside_kernel(length, me, pw, pr, pd, pc, aw, ar, ad, ac, *refs):
    chunks, (y_out, dx_out, dr_out, dw_out, adw, z_out, x, zs) = refs[:GROUP], refs[GROUP:]
    b = pl.program_id(0)
    answer = b == 2
    write = jnp.where(answer, aw[0], pw[0])
    read = jnp.where(answer, ar[0], pr[0])
    decay = jnp.where(answer, ad[0], pd[0])
    alive = jnp.where(answer, length[0], B)
    cot32 = live_rows(jnp.where(answer, ac[0], pc[0]).astype(F32), alive)
    cot_t = cot32.T.astype(BF16)
    assembled(me, chunks, x)
    rows = running_rows(decay)
    columns = running_columns(decay)
    scores = nt(read, write)
    causal = iota((B, B), 0) >= iota((B, B), 1)
    first = iota((B, 2 * HD), 1) < HD
    grad = jnp.zeros((B, B), F32)
    for pair in range(H // 2):
        lanes = slice(2 * HD * pair, 2 * HD * pair + 2 * HD)
        xs = x[:, lanes]
        cs = cot32[:, lanes]
        ys, dxs = [], []
        for s in range(2):
            h = 2 * pair + s
            gap = columns[:, h : h + 1] - rows[h : h + 1, :]
            weight = jnp.exp(jnp.where(causal, gap, -1e30))
            mixing = (weight * scores).astype(BF16)
            ys.append(nn(mixing, xs))
            dxs.append(nn(cot_t[HD * h : HD * h + HD, :], mixing))
            own = jnp.where(first if s == 0 else jnp.logical_not(first), cs, 0.0).astype(BF16)
            grad = grad + nt(own, xs) * weight
        y = jnp.where(first, ys[0], ys[1])
        dx = jnp.concatenate(dxs, axis=0).T
        y_out[0, :, lanes] = y.astype(BF16)
        dx_out[0, :, lanes] = dx.astype(BF16)
        zs[:, lanes] = cs * y - xs.astype(F32) * dx
    z_out[0] = head_sums(zs[...])
    grad = grad.astype(BF16)
    dr_out[0] = nn(grad, write)
    dw = tn(grad, read)

    @pl.when(b < 2)
    def _():
        dw_out[0] = dw

    @pl.when(answer)
    def _():
        adw[0] = dw.astype(BF16)


def token_kernel(me, m2, pw, pd, dxi, dwi, *refs):
    chunks, outs = refs[:GROUP], refs[GROUP : 2 * GROUP]
    pdw, z, closing, ends, full, x = refs[2 * GROUP :]
    b = pl.program_id(0)

    @pl.when(b < 2)
    def _():
        gathered(m2, ends)
        assembled(me, chunks, x)
        xs = x[...].astype(F32)
        to_close = closing_weight(pd[0])
        tail = nn(pw[0], ends[...]) * to_close
        full[...] = (dxi[0].astype(F32) + tail).astype(BF16)
        pdw[0] = (dwi[0] + nt((xs * to_close).astype(BF16), ends[...])).astype(BF16)
        tail = tail * xs
        closing[0] = jnp.broadcast_to(jnp.sum(tail, axis=0, keepdims=True), (8, L))
        z[0] = head_sums(tail)

    @pl.when(b == 2)
    def _():
        full[...] = dxi[0]

    for k in range(GROUP):
        there = pl.multiple_of((me[0] ^ k) * ROWS, ROWS)
        outs[k][0] = full[pl.ds(there, ROWS), :]


def output_kernel(
    length, m2, m3, pr, pd, pc, ar, ad, ac, yi, dri, zi, z, closing, py, pdr, pdd, ay, adr, add, start, ends
):
    b = pl.program_id(0)
    answer = b == 2
    gathered(m3, start)
    read = jnp.where(answer, ar[0], pr[0])
    decay = jnp.where(answer, ad[0], pd[0])
    alive = jnp.where(answer, length[0], B)
    cot = live_rows(jnp.where(answer, ac[0], pc[0]).astype(F32), alive)
    growth = grown(decay)
    outside = nn(read, start[...]) * growth
    y = yi[0].astype(F32) + outside
    dr = dri[0] + nt((cot * growth).astype(BF16), start[...])
    zs = zi[0] + head_sums(cot * outside) - jnp.where(answer, 0.0, z[0])
    tri = lower()
    dd = sum(tn(part, tri) for part in terms(zs))

    @pl.when(b < 2)
    def _():
        gathered(m2, ends)
        inner = jnp.sum(ends[...].astype(F32) * start[...].astype(F32), axis=0, keepdims=True)
        last = closing[0] + inner * growth[B - 1 : B, :]
        member = (iota((H, L), 1) // HD == iota((H, L), 0)).astype(BF16)
        total = sum(nt(member, part) for part in terms(last))
        py[0] = y.astype(BF16)
        pdr[0] = dr.astype(BF16)
        pdd[0] = dd + total[:, 0:1]

    @pl.when(answer)
    def _():
        ay[0] = live_rows(y, length[0]).astype(BF16)
        adr[0] = dr.astype(BF16)
        add[0] = dd


SMEM = pl.BlockSpec(memory_space=pltpu.SMEM)
VMEM = pl.BlockSpec(memory_space=pltpu.VMEM)
ANY = pl.BlockSpec(memory_space=pl.ANY)


def own(*dims):
    return pl.BlockSpec((1, *dims), lambda b: (jnp.minimum(b, 1), 0, 0))


def one(*dims):
    return pl.BlockSpec((1, *dims), lambda b: (0, 0, 0))


def each(*dims):
    return pl.BlockSpec((1, *dims), lambda b: (b, 0, 0))


def column(width, index):
    return pl.BlockSpec((B, width), lambda b: (0, index(b)))


def shape(dims, dtype=BF16):
    return jax.ShapeDtypeStruct(dims, dtype)


def call(kernel, steps, ins, outs, args, scratch=(), flops=1e9, alias=None, limit=None):
    return pl.pallas_call(
        kernel,
        grid=(steps,),
        in_specs=ins,
        out_specs=[spec for spec, _ in outs],
        out_shape=[struct for _, struct in outs],
        scratch_shapes=scratch,
        input_output_aliases=alias or {},
        compiler_params=pltpu.CompilerParams(vmem_limit_bytes=limit) if limit else None,
        cost_estimate=pl.CostEstimate(flops=int(flops), bytes_accessed=4000000, transcendentals=0),
    )(*args)


def exchange(chunks):
    sent = {0: chunks[0]}
    for offsets in ((4, 5), (2, 3, 6, 7), (1,)):
        for k in offsets:
            sent[k] = lax.ppermute(chunks[k], "head", [(i, i ^ k) for i in range(GROUP)])
    return [sent[k] for k in range(GROUP)]


def transposed(message):
    return lax.all_to_all(message, "seq", split_axis=0, concat_axis=0, tiled=True)


def per_device(pt, pw, pr, pd, pc, at, aw, ar, ad, ac, sizes, length):
    me = lax.axis_index("head").astype(jnp.int32).reshape(1)
    state = pltpu.VMEM((N, L), BF16)
    block = pltpu.VMEM((B, L), BF16)
    chunk = [(each(ROWS, L), shape((3, ROWS, L))) for _ in range(GROUP)]
    pieces = [each(ROWS, L)] * GROUP
    prompt_side = [own(B, N), own(H, B), own(B, L)]
    answer_side = [one(B, N), one(H, B), one(B, L)]
    (m1,) = call(
        reach_kernel,
        3,
        [SMEM, *prompt_side, *answer_side],
        [(column(3 * HALF + N, lambda b: 0), shape((B, 3 * HALF + N)))],
        (length, pr, pd, pc, ar, ad, ac),
        (pltpu.VMEM((8, L), F32),),
    )
    m1 = transposed(m1)
    cut = call(
        split_kernel,
        1,
        [SMEM, ANY, ANY],
        [(ANY, shape((3, ROWS, L)))] * GROUP,
        (me, pt, at),
        (
            pltpu.VMEM((GROUP, 3, ROWS, L), BF16),
            pltpu.SemaphoreType.DMA((2 * GROUP,)),
            pltpu.SemaphoreType.DMA((GROUP,)),
        ),
    )
    cut = exchange(cut)
    m2, factors = call(
        turn_kernel,
        1,
        [SMEM, column(2 * HALF, lambda q: 0), column(HALF, lambda q: 2), column(N, lambda q: 12)],
        [
            (column(2 * HALF, lambda q: 0), shape((B, 4 * HALF))),
            (pl.BlockSpec((2 * SHARDS, HALF), lambda q: (0, 0)), shape((2 * SHARDS, HALF), F32)),
        ],
        (sizes, m1, m1, m1),
    )
    (m2,) = call(
        local_kernel,
        2,
        [SMEM, ANY, each(B, N), each(H, B), *pieces],
        [(column(HALF, lambda q: 2 + q), shape((B, 4 * HALF)))],
        (me, m2, pw, pd, *cut),
        (block,),
        alias={1: 0},
    )
    m2 = transposed(m2)
    yi, dxi, dri, dwi, adw, zi = call(
        inside_kernel,
        3,
        [SMEM, SMEM, own(B, N), *prompt_side, one(B, N), *answer_side, *pieces],
        [
            (each(B, L), shape((3, B, L))),
            (each(B, L), shape((3, B, L))),
            (each(B, N), shape((3, B, N), F32)),
            (own(B, N), shape((2, B, N), F32)),
            (one(B, N), shape((1, B, N))),
            (each(B, H), shape((3, B, H), F32)),
        ],
        (length, me, pw, pr, pd, pc, aw, ar, ad, ac, *cut),
        (block, pltpu.VMEM((B, L), F32)),
        8e9,
    )
    (m3,) = call(
        start_kernel,
        1,
        [SMEM, VMEM, VMEM],
        [(VMEM, shape((B, 3 * HALF)))],
        (sizes, factors, m2),
        limit=4 << 20,
    )
    m3 = transposed(m3)
    made = call(
        token_kernel,
        3,
        [
            SMEM,
            column(HALF, lambda b: jnp.minimum(b, 1)),
            own(B, N),
            own(H, B),
            each(B, L),
            own(B, N),
            *[own(ROWS, L)] * GROUP,
        ],
        [
            *chunk,
            (own(B, N), shape((2, B, N))),
            (own(B, H), shape((2, B, H), F32)),
            (own(8, L), shape((2, 8, L), F32)),
        ],
        (me, m2, pw, pd, dxi, dwi, *cut),
        (state, block, block),
    )
    pdw, z, closing = made[GROUP:]
    back = exchange(made[:GROUP])
    py, pdr, pdd, ay, adr, add = call(
        output_kernel,
        3,
        [
            SMEM,
            column(HALF, lambda b: jnp.minimum(b, 1)),
            column(HALF, lambda b: b),
            *prompt_side,
            *answer_side,
            each(B, L),
            each(B, N),
            each(B, H),
            own(B, H),
            own(8, L),
        ],
        [
            (own(B, L), shape((2, B, L))),
            (own(B, N), shape((2, B, N))),
            (own(H, B), shape((2, H, B), F32)),
            (one(B, L), shape((1, B, L))),
            (one(B, N), shape((1, B, N))),
            (one(H, B), shape((1, H, B), F32)),
        ],
        (length, m2, m3, pr, pd, pc, ar, ad, ac, yi, dri, zi, z, closing),
        (state, state),
    )
    pdx, adx = call(
        join_kernel,
        1,
        [SMEM] + [ANY] * GROUP,
        [(ANY, shape((2, ROWS, GROUP * L))), (ANY, shape((1, ROWS, GROUP * L)))],
        (me, *back),
        (
            pltpu.VMEM((GROUP, 3, ROWS, L), BF16),
            pltpu.SemaphoreType.DMA((GROUP,)),
            pltpu.SemaphoreType.DMA((2 * GROUP,)),
        ),
    )
    return py, pdx, pdw, pdr, pdd, ay, adx, adw, adr, add


def solution(mesh):
    split_positions = P(None, ("seq", "head"), None)
    prompt = P(None, "seq", "head")
    answer = P("seq", None, "head")
    return jax.shard_map(
        per_device,
        mesh=mesh,
        in_specs=(
            split_positions,
            prompt,
            prompt,
            P(None, "head", "seq"),
            prompt,
            P("seq", "head", None),
            answer,
            answer,
            P("seq", "head", None),
            answer,
            P(),
            P("seq"),
        ),
        out_specs=(
            prompt,
            split_positions,
            prompt,
            prompt,
            P(None, "head", "seq"),
            answer,
            P("seq", "head", None),
            answer,
            answer,
            P("seq", "head", None),
        ),
        check_vma=False,
    )
```

```python
import jax
import jax.numpy as jnp
from jax import lax
from jax.experimental import pallas as pl
from jax.experimental.pallas import tpu as pltpu
from jax.sharding import PartitionSpec as P


HD = 64
N = 128
B = 256
H = 16
L = H * HD
SHARDS = 16
GROUP = 8
ROWS = B // GROUP
HALF = L // 2
F32 = jnp.float32
BF16 = jnp.bfloat16


def nn(a, b):
    return lax.dot_general(a, b, (((1,), (0,)), ((), ())), preferred_element_type=F32)


def nt(a, b):
    return lax.dot_general(a, b, (((1,), (1,)), ((), ())), preferred_element_type=F32)


def tn(a, b):
    return lax.dot_general(a, b, (((0,), (0,)), ((), ())), preferred_element_type=F32)


def iota(shape, axis):
    return lax.broadcasted_iota(jnp.int32, shape, axis)


def terms(value):
    high = value.astype(BF16)
    rest = value - high.astype(F32)
    middle = rest.astype(BF16)
    return high, middle, (rest - middle.astype(F32)).astype(BF16)


def upper():
    return (iota((B, B), 0) <= iota((B, B), 1)).astype(BF16)


def lower():
    return (iota((B, B), 1) <= iota((B, B), 0)).astype(BF16)


def running_rows(decay):
    parts = nn(jnp.concatenate([part.astype(F32) for part in terms(decay)], axis=0).astype(BF16), upper())
    return parts[:H] + parts[H : 2 * H] + parts[2 * H :]


def running_columns(decay):
    tri = lower()
    total = None
    for part in terms(decay):
        wide = part.astype(F32)
        added = nt(tri, jnp.concatenate([wide, wide, wide], axis=0).astype(BF16))
        total = added if total is None else total + added
    return total


def widened(columns):
    lane = iota(columns.shape, 1)
    high = columns.astype(BF16).astype(F32)
    rest = columns - high
    middle = rest.astype(BF16).astype(F32)
    packed = jnp.where(lane < H, high, jnp.where(lane < 2 * H, middle, rest - middle)).astype(BF16)
    member = (iota((3 * H, L), 1) // HD == iota((3 * H, L), 0) % H).astype(BF16)
    return nn(packed, member)


def grown(decay):
    return widened(jnp.exp(running_columns(decay)))


def closing_weight(decay):
    columns = running_columns(decay)
    return widened(jnp.exp(columns[B - 1 : B, :] - columns))


def head_sums(values):
    member = (iota((H, L), 1) // HD == iota((H, L), 0)).astype(BF16)
    high = values.astype(BF16)
    low = (values - high.astype(F32)).astype(BF16)
    return nt(member, high) + nt(member, low)


def live_rows(value, length):
    return jnp.where(iota(value.shape, 0) < length, value, jnp.zeros_like(value))


def piece(d):
    return slice(16 * (d // 2), 16 * (d // 2) + 16), slice(HALF * (d % 2), HALF * (d % 2) + HALF)


def scattered(out, state, first):
    for d in range(SHARDS):
        rows, lanes = piece(d)
        out[16 * d : 16 * d + 16, pl.ds(first, HALF)] = state[rows, lanes].astype(BF16)


def gathered(m, place):
    for d in range(SHARDS):
        rows, lanes = piece(d)
        place[rows, lanes] = m[16 * d : 16 * d + 16, :]


def assembled(me, chunks, x):
    for k in range(GROUP):
        there = pl.multiple_of((me[0] ^ k) * ROWS, ROWS)
        x[pl.ds(there, ROWS), :] = chunks[k][0]


def reach_kernel(length, pr, pd, pc, ar, ad, ac, out, reads, decays, cots, stage, factors, came, went):
    coming = []
    for b in range(3):
        group = []
        for i, (prompt, answer, place) in enumerate(((pd, ad, decays), (pr, ar, reads), (pc, ac, cots))):
            source = prompt.at[b] if b < 2 else answer.at[0]
            group.append(pltpu.make_async_copy(source, place.at[b], came.at[3 * b + i]))
            group[-1].start()
        coming.append(group)
    going = []
    for b in range(3):
        for copy in coming[b]:
            copy.wait()
        cot = cots[b].astype(F32)
        if b == 2:
            cot = live_rows(cot, length[0])
        growth = grown(decays[b])
        scattered(stage, tn(reads[b], (cot * growth).astype(BF16)), b * HALF)
        going.append(pltpu.make_async_copy(stage.at[:, pl.ds(b * HALF, HALF)], out.at[:, pl.ds(b * HALF, HALF)], went.at[b]))
        going[-1].start()
        if b < 2:
            last = growth[B - 1 : B, :]
            high = last.astype(BF16).astype(F32)
            factors[2 * b : 2 * b + 1, :] = high
            factors[2 * b + 1 : 2 * b + 2, :] = last - high
        if b == 1:
            for half in range(2):
                lanes = [slice(HALF * half + N * j, HALF * half + N * j + N) for j in range(4)]
                part = jnp.concatenate([factors[i : i + 1, lane] for i in range(4) for lane in lanes], axis=0)
                for d in range(half, SHARDS, 2):
                    stage[16 * d : 16 * d + 16, 3 * HALF :] = part.astype(BF16)
            tail = pl.ds(3 * HALF, N)
            going.append(pltpu.make_async_copy(stage.at[:, tail], out.at[:, tail], went.at[3]))
            going[-1].start()
    for copy in going:
        copy.wait()


def split_kernel(me, pt, at, *refs):
    outs, came = refs[:GROUP], refs[GROUP]
    copies = []
    for k in range(GROUP):
        there = pl.multiple_of((me[0] ^ k) * L, L)
        copies.append(pltpu.make_async_copy(pt.at[:, :, pl.ds(there, L)], outs[k].at[0:2], came.at[2 * k]))
        copies.append(pltpu.make_async_copy(at.at[:, :, pl.ds(there, L)], outs[k].at[2:3], came.at[2 * k + 1]))
    for copy in copies:
        copy.start()
    for copy in copies:
        copy.wait()


def join_kernel(me, *refs):
    ins, (pt, at, went) = refs[:GROUP], refs[GROUP:]
    copies = []
    for k in range(GROUP):
        there = pl.multiple_of((me[0] ^ k) * L, L)
        copies.append(pltpu.make_async_copy(ins[k].at[0:2], pt.at[:, :, pl.ds(there, L)], went.at[2 * k]))
        copies.append(pltpu.make_async_copy(ins[k].at[2:3], at.at[:, :, pl.ds(there, L)], went.at[2 * k + 1]))
    for copy in copies:
        copy.start()
    for copy in copies:
        copy.wait()


def shard_factor(packed, k, q):
    part = packed[16 * k : 16 * k + 16, :].astype(F32)
    rows = [part[8 * q + j : 8 * q + j + 1] + part[8 * q + 4 + j : 8 * q + 5 + j] for j in range(4)]
    return jnp.concatenate(rows, axis=1)


def owner_of(sizes, k):
    return (sizes[0] <= k).astype(jnp.int32) + (sizes[0] + sizes[1] <= k).astype(jnp.int32)


def local_kernel(me, message, pw, pd, *refs):
    chunks, (out, x) = refs[:GROUP], refs[GROUP:]
    assembled(me, chunks, x)
    weighted = (x[...].astype(F32) * closing_weight(pd[0])).astype(BF16)
    scattered(out, tn(pw[0], weighted), 0)


def turn_kernel(sizes, reach, answers, packed, out, factors):
    for q in range(2):
        grad = jnp.zeros((16, HALF), F32)
        for k in range(SHARDS):
            part = answers[16 * k : 16 * k + 16, :].astype(F32)
            grad = grad + part * (owner_of(sizes, k) == q).astype(F32)
        for k in reversed(range(SHARDS)):
            out[16 * k : 16 * k + 16, q * HALF : (q + 1) * HALF] = grad.astype(BF16)
            factor = shard_factor(packed, k, q)
            factors[16 * q + k : 16 * q + k + 1, :] = factor
            grad = reach[16 * k : 16 * k + 16, q * HALF : (q + 1) * HALF].astype(F32) + factor * grad


def start_kernel(sizes, factors, m2, out):
    ends = []
    for q in range(2):
        state = jnp.zeros((16, HALF), F32)
        for k in range(SHARDS):
            out[16 * k : 16 * k + 16, q * HALF : (q + 1) * HALF] = state.astype(BF16)
            local = m2[16 * k : 16 * k + 16, (2 + q) * HALF : (3 + q) * HALF].astype(F32)
            state = factors[16 * q + k : 16 * q + k + 1, :] * state + local
        ends.append(state)
    for k in range(SHARDS):
        owner = owner_of(sizes, k)
        mine = ends[0] * (owner == 0).astype(F32) + ends[1] * (owner == 1).astype(F32)
        out[16 * k : 16 * k + 16, 2 * HALF : 3 * HALF] = mine.astype(BF16)


def inside_kernel(length, me, pw, pr, pd, pc, aw, ar, ad, ac, *refs):
    chunks, outs = refs[:GROUP], refs[GROUP : 2 * GROUP]
    y_out, dx_out, dr_out, dw_out, adw, z_out, x, zs, full = refs[2 * GROUP :]
    b = pl.program_id(0)
    answer = b == 2
    write = jnp.where(answer, aw[0], pw[0])
    read = jnp.where(answer, ar[0], pr[0])
    decay = jnp.where(answer, ad[0], pd[0])
    alive = jnp.where(answer, length[0], B)
    cot32 = live_rows(jnp.where(answer, ac[0], pc[0]).astype(F32), alive)
    cot_t = cot32.T.astype(BF16)
    assembled(me, chunks, x)
    rows = running_rows(decay)
    columns = running_columns(decay)
    scores = nt(read, write)
    causal = iota((B, B), 0) >= iota((B, B), 1)
    first = iota((B, 2 * HD), 1) < HD
    grad = jnp.zeros((B, B), F32)
    for pair in range(H // 2):
        lanes = slice(2 * HD * pair, 2 * HD * pair + 2 * HD)
        xs = x[:, lanes]
        cs = cot32[:, lanes]
        ys, dxs = [], []
        for s in range(2):
            h = 2 * pair + s
            gap = columns[:, h : h + 1] - rows[h : h + 1, :]
            weight = jnp.exp(jnp.where(causal, gap, -1e30))
            mixing = (weight * scores).astype(BF16)
            ys.append(nn(mixing, xs))
            dxs.append(nn(cot_t[HD * h : HD * h + HD, :], mixing))
            own = jnp.where(first if s == 0 else jnp.logical_not(first), cs, 0.0).astype(BF16)
            grad = grad + nt(own, xs) * weight
        y = jnp.where(first, ys[0], ys[1])
        dx = jnp.concatenate(dxs, axis=0).T
        y_out[0, :, lanes] = y.astype(BF16)
        full[:, lanes] = dx.astype(BF16)
        zs[:, lanes] = cs * y - xs.astype(F32) * dx
    z_out[0] = head_sums(zs[...])
    grad = grad.astype(BF16)
    dr_out[0] = nn(grad, write)
    dw = tn(grad, read)

    @pl.when(b < 2)
    def _():
        dx_out[0] = full[...]
        dw_out[0] = dw

    @pl.when(answer)
    def _():
        adw[0] = dw.astype(BF16)
        for k in range(GROUP):
            there = pl.multiple_of((me[0] ^ k) * ROWS, ROWS)
            outs[k][0] = full[pl.ds(there, ROWS), :]


def token_kernel(me, m2, pw, pd, dxi, dwi, *refs):
    chunks, outs = refs[:GROUP], refs[2 * GROUP : 3 * GROUP]
    pdw, z, closing, ends, full, x = refs[3 * GROUP :]
    gathered(m2, ends)
    assembled(me, chunks, x)
    xs = x[...].astype(F32)
    to_close = closing_weight(pd[0])
    tail = nn(pw[0], ends[...]) * to_close
    full[...] = (dxi[0].astype(F32) + tail).astype(BF16)
    pdw[0] = (dwi[0] + nt((xs * to_close).astype(BF16), ends[...])).astype(BF16)
    tail = tail * xs
    closing[0] = jnp.broadcast_to(jnp.sum(tail, axis=0, keepdims=True), (8, L))
    z[0] = head_sums(tail)
    for k in range(GROUP):
        there = pl.multiple_of((me[0] ^ k) * ROWS, ROWS)
        outs[k][0] = full[pl.ds(there, ROWS), :]


def output_kernel(
    length, m2, m3, pr, pd, pc, ar, ad, ac, yi, dri, zi, z, closing, py, pdr, pdd, ay, adr, add, start, ends
):
    b = pl.program_id(0)
    answer = b == 2
    gathered(m3, start)
    read = jnp.where(answer, ar[0], pr[0])
    decay = jnp.where(answer, ad[0], pd[0])
    alive = jnp.where(answer, length[0], B)
    cot = live_rows(jnp.where(answer, ac[0], pc[0]).astype(F32), alive)
    growth = grown(decay)
    outside = nn(read, start[...]) * growth
    y = yi[0].astype(F32) + outside
    dr = dri[0] + nt((cot * growth).astype(BF16), start[...])
    zs = zi[0] + head_sums(cot * outside) - jnp.where(answer, 0.0, z[0])
    tri = lower()
    dd = sum(nn(part, tri) for part in terms(zs))

    @pl.when(b < 2)
    def _():
        gathered(m2, ends)
        inner = jnp.sum(ends[...].astype(F32) * start[...].astype(F32), axis=0, keepdims=True)
        last = closing[0] + inner * growth[B - 1 : B, :]
        member = (iota((H, L), 1) // HD == iota((H, L), 0)).astype(BF16)
        total = sum(nt(member, part) for part in terms(last))
        py[0] = y.astype(BF16)
        pdr[0] = dr.astype(BF16)
        pdd[0] = dd + total[:, 0:1]

    @pl.when(answer)
    def _():
        ay[0] = live_rows(y, length[0]).astype(BF16)
        adr[0] = dr.astype(BF16)
        add[0] = dd


SMEM = pl.BlockSpec(memory_space=pltpu.SMEM)
VMEM = pl.BlockSpec(memory_space=pltpu.VMEM)
ANY = pl.BlockSpec(memory_space=pl.ANY)


def own(*dims):
    return pl.BlockSpec((1, *dims), lambda b: (jnp.minimum(b, 1), 0, 0))


def one(*dims):
    return pl.BlockSpec((1, *dims), lambda b: (0, 0, 0))


def each(*dims):
    return pl.BlockSpec((1, *dims), lambda b: (b, 0, 0))


def column(width, index):
    return pl.BlockSpec((B, width), lambda b: (0, index(b)))


def shape(dims, dtype=BF16):
    return jax.ShapeDtypeStruct(dims, dtype)


def call(kernel, steps, ins, outs, args, scratch=(), flops=1e9, alias=None, limit=None):
    return pl.pallas_call(
        kernel,
        grid=(steps,),
        in_specs=ins,
        out_specs=[spec for spec, _ in outs],
        out_shape=[struct for _, struct in outs],
        scratch_shapes=scratch,
        input_output_aliases=alias or {},
        compiler_params=pltpu.CompilerParams(vmem_limit_bytes=limit) if limit else None,
        cost_estimate=pl.CostEstimate(flops=int(flops), bytes_accessed=4000000, transcendentals=0),
    )(*args)


def exchange(chunks):
    sent = {0: chunks[0]}
    for offsets in ((4, 5), (2, 3, 6, 7), (1,)):
        for k in offsets:
            sent[k] = lax.ppermute(chunks[k], "head", [(i, i ^ k) for i in range(GROUP)])
    return [sent[k] for k in range(GROUP)]


def transposed(message):
    return lax.all_to_all(message, "seq", split_axis=0, concat_axis=0, tiled=True)


def per_device(pt, pw, pr, pd, pc, at, aw, ar, ad, ac, sizes, length):
    me = lax.axis_index("head").astype(jnp.int32).reshape(1)
    state = pltpu.VMEM((N, L), BF16)
    block = pltpu.VMEM((B, L), BF16)
    chunk = [(each(ROWS, L), shape((3, ROWS, L))) for _ in range(GROUP)]
    pieces = [each(ROWS, L)] * GROUP
    prompt_side = [own(B, N), own(H, B), own(B, L)]
    answer_side = [one(B, N), one(H, B), one(B, L)]
    (m1,) = call(
        reach_kernel,
        1,
        [SMEM] + [ANY] * 6,
        [(ANY, shape((B, 3 * HALF + N)))],
        (length, pr, pd, pc, ar, ad, ac),
        (
            pltpu.VMEM((3, B, N), BF16),
            pltpu.VMEM((3, H, B), F32),
            pltpu.VMEM((3, B, L), BF16),
            pltpu.VMEM((B, 3 * HALF + N), BF16),
            pltpu.VMEM((8, L), F32),
            pltpu.SemaphoreType.DMA((9,)),
            pltpu.SemaphoreType.DMA((4,)),
        ),
    )
    m1 = transposed(m1)
    cut = call(
        split_kernel,
        1,
        [SMEM, ANY, ANY],
        [(VMEM, shape((3, ROWS, L)))] * GROUP,
        (me, pt, at),
        (
            pltpu.SemaphoreType.DMA((2 * GROUP,)),
        ),
        limit=4 << 20,
    )
    cut = exchange(cut)
    m2, factors = call(
        turn_kernel,
        1,
        [SMEM, column(2 * HALF, lambda q: 0), column(HALF, lambda q: 2), column(N, lambda q: 12)],
        [
            (column(2 * HALF, lambda q: 0), shape((B, 4 * HALF))),
            (pl.BlockSpec((2 * SHARDS, HALF), lambda q: (0, 0)), shape((2 * SHARDS, HALF), F32)),
        ],
        (sizes, m1, m1, m1),
        limit=8 << 20,
    )
    (m2,) = call(
        local_kernel,
        2,
        [SMEM, ANY, each(B, N), each(H, B), *pieces],
        [(column(HALF, lambda q: 2 + q), shape((B, 4 * HALF)))],
        (me, m2, pw, pd, *cut),
        (block,),
        alias={1: 0},
        limit=12 << 20,
    )
    m2 = transposed(m2)
    made = call(
        inside_kernel,
        3,
        [SMEM, SMEM, own(B, N), *prompt_side, one(B, N), *answer_side, *pieces],
        [
            *[(pl.BlockSpec((1, ROWS, L), lambda b: (2, 0, 0)), shape((3, ROWS, L)))] * GROUP,
            (each(B, L), shape((3, B, L))),
            (own(B, L), shape((2, B, L))),
            (each(B, N), shape((3, B, N), F32)),
            (own(B, N), shape((2, B, N), F32)),
            (one(B, N), shape((1, B, N))),
            (each(H, B), shape((3, H, B), F32)),
        ],
        (length, me, pw, pr, pd, pc, aw, ar, ad, ac, *cut),
        (block, pltpu.VMEM((B, L), F32), block),
        8e9,
    )
    yi, dxi, dri, dwi, adw, zi = made[GROUP:]
    (m3,) = call(
        start_kernel, 1, [SMEM, VMEM, VMEM], [(VMEM, shape((B, 3 * HALF)))], (sizes, factors, m2), limit=4 << 20
    )
    m3 = transposed(m3)
    made = call(
        token_kernel,
        2,
        [SMEM, column(HALF, lambda q: q), each(B, N), each(H, B), each(B, L), each(B, N), *pieces, *[ANY] * GROUP],
        [
            *chunk,
            (each(B, N), shape((2, B, N))),
            (each(H, B), shape((2, H, B), F32)),
            (each(8, L), shape((2, 8, L), F32)),
        ],
        (me, m2, pw, pd, dxi, dwi, *cut, *made[:GROUP]),
        (state, block, block),
        alias={6 + GROUP + k: k for k in range(GROUP)},
    )
    pdw, z, closing = made[GROUP:]
    back = exchange(made[:GROUP])
    py, pdr, pdd, ay, adr, add = call(
        output_kernel,
        3,
        [
            SMEM,
            column(HALF, lambda b: jnp.minimum(b, 1)),
            column(HALF, lambda b: b),
            *prompt_side,
            *answer_side,
            each(B, L),
            each(B, N),
            each(H, B),
            own(H, B),
            own(8, L),
        ],
        [
            (own(B, L), shape((2, B, L))),
            (own(B, N), shape((2, B, N))),
            (own(H, B), shape((2, H, B), F32)),
            (one(B, L), shape((1, B, L))),
            (one(B, N), shape((1, B, N))),
            (one(H, B), shape((1, H, B), F32)),
        ],
        (length, m2, m3, pr, pd, pc, ar, ad, ac, yi, dri, zi, z, closing),
        (state, state),
    )
    pdx, adx = call(
        join_kernel,
        1,
        [SMEM] + [VMEM] * GROUP,
        [(ANY, shape((2, ROWS, GROUP * L))), (ANY, shape((1, ROWS, GROUP * L)))],
        (me, *back),
        (
            pltpu.SemaphoreType.DMA((2 * GROUP,)),
        ),
        limit=4 << 20,
    )
    return py, pdx, pdw, pdr, pdd, ay, adx, adw, adr, add


def solution(mesh):
    split_positions = P(None, ("seq", "head"), None)
    prompt = P(None, "seq", "head")
    answer = P("seq", None, "head")
    return jax.shard_map(
        per_device,
        mesh=mesh,
        in_specs=(
            split_positions,
            prompt,
            prompt,
            P(None, "head", "seq"),
            prompt,
            P("seq", "head", None),
            answer,
            answer,
            P("seq", "head", None),
            answer,
            P(),
            P("seq"),
        ),
        out_specs=(
            prompt,
            split_positions,
            prompt,
            prompt,
            P(None, "head", "seq"),
            answer,
            P("seq", "head", None),
            answer,
            answer,
            P("seq", "head", None),
        ),
        check_vma=False,
    )
```

```python
import jax
import jax.numpy as jnp
from jax import lax
from jax.experimental import pallas as pl
from jax.experimental.pallas import tpu as pltpu
from jax.sharding import PartitionSpec as P


HD = 64
N = 128
B = 256
H = 16
L = H * HD
SHARDS = 16
GROUP = 8
ROWS = B // GROUP
HALF = L // 2
F32 = jnp.float32
BF16 = jnp.bfloat16


def nn(a, b):
    return lax.dot_general(a, b, (((1,), (0,)), ((), ())), preferred_element_type=F32)


def nt(a, b):
    return lax.dot_general(a, b, (((1,), (1,)), ((), ())), preferred_element_type=F32)


def tn(a, b):
    return lax.dot_general(a, b, (((0,), (0,)), ((), ())), preferred_element_type=F32)


def iota(shape, axis):
    return lax.broadcasted_iota(jnp.int32, shape, axis)


def terms(value):
    high = value.astype(BF16)
    rest = value - high.astype(F32)
    middle = rest.astype(BF16)
    return high, middle, (rest - middle.astype(F32)).astype(BF16)


def upper():
    return (iota((B, B), 0) <= iota((B, B), 1)).astype(BF16)


def lower():
    return (iota((B, B), 1) <= iota((B, B), 0)).astype(BF16)


def running_rows(decay):
    parts = nn(jnp.concatenate([part.astype(F32) for part in terms(decay)], axis=0).astype(BF16), upper())
    return parts[:H] + parts[H : 2 * H] + parts[2 * H :]


def running_columns(decay):
    tri = lower()
    total = None
    for part in terms(decay):
        wide = part.astype(F32)
        added = nt(tri, jnp.concatenate([wide, wide, wide], axis=0).astype(BF16))
        total = added if total is None else total + added
    return total


def widened(columns):
    lane = iota(columns.shape, 1)
    high = columns.astype(BF16).astype(F32)
    rest = columns - high
    middle = rest.astype(BF16).astype(F32)
    packed = jnp.where(lane < H, high, jnp.where(lane < 2 * H, middle, rest - middle)).astype(BF16)
    member = (iota((3 * H, L), 1) // HD == iota((3 * H, L), 0) % H).astype(BF16)
    return nn(packed, member)


def grown(decay):
    return widened(jnp.exp(running_columns(decay)))


def closing_weight(decay):
    columns = running_columns(decay)
    return widened(jnp.exp(columns[B - 1 : B, :] - columns))


def head_sums(values):
    member = (iota((H, L), 1) // HD == iota((H, L), 0)).astype(BF16)
    high = values.astype(BF16)
    low = (values - high.astype(F32)).astype(BF16)
    return nt(member, high) + nt(member, low)


def live_rows(value, length):
    return jnp.where(iota(value.shape, 0) < length, value, jnp.zeros_like(value))


def piece(d):
    return slice(16 * (d // 2), 16 * (d // 2) + 16), slice(HALF * (d % 2), HALF * (d % 2) + HALF)


def scattered(out, state, first):
    for d in range(SHARDS):
        rows, lanes = piece(d)
        out[16 * d : 16 * d + 16, pl.ds(first, HALF)] = state[rows, lanes].astype(BF16)


def gathered(m, place):
    for d in range(SHARDS):
        rows, lanes = piece(d)
        place[rows, lanes] = m[16 * d : 16 * d + 16, :]


def assembled(me, chunks, x):
    for k in range(GROUP):
        there = pl.multiple_of((me[0] ^ k) * ROWS, ROWS)
        x[pl.ds(there, ROWS), :] = chunks[k][0]


def reach_kernel(length, pr, pd, pc, ar, ad, ac, out, done, reads, decays, cots, stage, factors, came, went):
    done[...] = jnp.zeros((8, N), F32)
    coming = []
    for b in range(3):
        group = []
        for i, (prompt, answer, place) in enumerate(((pd, ad, decays), (pr, ar, reads), (pc, ac, cots))):
            source = prompt.at[b] if b < 2 else answer.at[0]
            group.append(pltpu.make_async_copy(source, place.at[b], came.at[3 * b + i]))
            group[-1].start()
        coming.append(group)
    going = []
    for b in range(3):
        for copy in coming[b]:
            copy.wait()
        cot = cots[b].astype(F32)
        if b == 2:
            cot = live_rows(cot, length[0])
        growth = grown(decays[b])
        scattered(stage, tn(reads[b], (cot * growth).astype(BF16)), b * HALF)
        going.append(pltpu.make_async_copy(stage.at[:, pl.ds(b * HALF, HALF)], out.at[:, pl.ds(b * HALF, HALF)], went.at[b]))
        going[-1].start()
        if b < 2:
            last = growth[B - 1 : B, :]
            high = last.astype(BF16).astype(F32)
            factors[2 * b : 2 * b + 1, :] = high
            factors[2 * b + 1 : 2 * b + 2, :] = last - high
        if b == 1:
            for half in range(2):
                lanes = [slice(HALF * half + N * j, HALF * half + N * j + N) for j in range(4)]
                part = jnp.concatenate([factors[i : i + 1, lane] for i in range(4) for lane in lanes], axis=0)
                for d in range(half, SHARDS, 2):
                    stage[16 * d : 16 * d + 16, 3 * HALF :] = part.astype(BF16)
            tail = pl.ds(3 * HALF, N)
            going.append(pltpu.make_async_copy(stage.at[:, tail], out.at[:, tail], went.at[3]))
            going[-1].start()
    for copy in going:
        copy.wait()


def split_kernel(me, pt, at, done, *refs):
    outs, came = refs[:GROUP], refs[GROUP]
    copies = []
    for k in range(GROUP):
        there = pl.multiple_of((me[0] ^ k) * L, L)
        copies.append(pltpu.make_async_copy(pt.at[:, :, pl.ds(there, L)], outs[k].at[0:2], came.at[2 * k]))
        copies.append(pltpu.make_async_copy(at.at[:, :, pl.ds(there, L)], outs[k].at[2:3], came.at[2 * k + 1]))
    for copy in copies:
        copy.start()
    for copy in copies:
        copy.wait()


def join_kernel(me, *refs):
    ins, (pt, at, went) = refs[:GROUP], refs[GROUP:]
    copies = []
    for k in range(GROUP):
        there = pl.multiple_of((me[0] ^ k) * L, L)
        copies.append(pltpu.make_async_copy(ins[k].at[0:2], pt.at[:, :, pl.ds(there, L)], went.at[2 * k]))
        copies.append(pltpu.make_async_copy(ins[k].at[2:3], at.at[:, :, pl.ds(there, L)], went.at[2 * k + 1]))
    for copy in copies:
        copy.start()
    for copy in copies:
        copy.wait()


def shard_factor(packed, k, q):
    part = packed[16 * k : 16 * k + 16, :].astype(F32)
    rows = [part[8 * q + j : 8 * q + j + 1] + part[8 * q + 4 + j : 8 * q + 5 + j] for j in range(4)]
    return jnp.concatenate(rows, axis=1)


def owner_of(sizes, k):
    return (sizes[0] <= k).astype(jnp.int32) + (sizes[0] + sizes[1] <= k).astype(jnp.int32)


def local_kernel(me, message, pw, pd, *refs):
    chunks, (out, x) = refs[:GROUP], refs[GROUP:]
    assembled(me, chunks, x)
    weighted = (x[...].astype(F32) * closing_weight(pd[0])).astype(BF16)
    scattered(out, tn(pw[0], weighted), 0)


def turn_kernel(sizes, reach, answers, packed, out, factors):
    for q in range(2):
        grad = jnp.zeros((16, HALF), F32)
        for k in range(SHARDS):
            part = answers[16 * k : 16 * k + 16, :].astype(F32)
            grad = grad + part * (owner_of(sizes, k) == q).astype(F32)
        for k in reversed(range(SHARDS)):
            out[16 * k : 16 * k + 16, q * HALF : (q + 1) * HALF] = grad.astype(BF16)
            factor = shard_factor(packed, k, q)
            factors[16 * q + k : 16 * q + k + 1, :] = factor
            grad = reach[16 * k : 16 * k + 16, q * HALF : (q + 1) * HALF].astype(F32) + factor * grad


def start_kernel(sizes, factors, m2, out):
    ends = []
    for q in range(2):
        state = jnp.zeros((16, HALF), F32)
        for k in range(SHARDS):
            out[16 * k : 16 * k + 16, q * HALF : (q + 1) * HALF] = state.astype(BF16)
            local = m2[16 * k : 16 * k + 16, (2 + q) * HALF : (3 + q) * HALF].astype(F32)
            state = factors[16 * q + k : 16 * q + k + 1, :] * state + local
        ends.append(state)
    for k in range(SHARDS):
        owner = owner_of(sizes, k)
        mine = ends[0] * (owner == 0).astype(F32) + ends[1] * (owner == 1).astype(F32)
        out[16 * k : 16 * k + 16, 2 * HALF : 3 * HALF] = mine.astype(BF16)


def inside_kernel(length, me, pw, pr, pd, pc, aw, ar, ad, ac, *refs):
    chunks, outs = refs[:GROUP], refs[GROUP : 2 * GROUP]
    y_out, dx_out, dr_out, dw_out, adw, z_out, x, zs, full = refs[2 * GROUP :]
    b = pl.program_id(0)
    answer = b == 2
    write = jnp.where(answer, aw[0], pw[0])
    read = jnp.where(answer, ar[0], pr[0])
    decay = jnp.where(answer, ad[0], pd[0])
    alive = jnp.where(answer, length[0], B)
    cot32 = live_rows(jnp.where(answer, ac[0], pc[0]).astype(F32), alive)
    cot_t = cot32.T.astype(BF16)
    assembled(me, chunks, x)
    rows = running_rows(decay)
    columns = running_columns(decay)
    scores = nt(read, write)
    causal = iota((B, B), 0) >= iota((B, B), 1)
    first = iota((B, 2 * HD), 1) < HD
    grad = jnp.zeros((B, B), F32)
    for pair in range(H // 2):
        lanes = slice(2 * HD * pair, 2 * HD * pair + 2 * HD)
        xs = x[:, lanes]
        cs = cot32[:, lanes]
        ys, dxs = [], []
        for s in range(2):
            h = 2 * pair + s
            gap = columns[:, h : h + 1] - rows[h : h + 1, :]
            weight = jnp.exp(jnp.where(causal, gap, -1e30))
            mixing = (weight * scores).astype(BF16)
            ys.append(nn(mixing, xs))
            dxs.append(nn(cot_t[HD * h : HD * h + HD, :], mixing))
            own = jnp.where(first if s == 0 else jnp.logical_not(first), cs, 0.0).astype(BF16)
            grad = grad + nt(own, xs) * weight
        y = jnp.where(first, ys[0], ys[1])
        dx = jnp.concatenate(dxs, axis=0).T
        y_out[0, :, lanes] = y.astype(BF16)
        full[:, lanes] = dx.astype(BF16)
        zs[:, lanes] = cs * y - xs.astype(F32) * dx
    z_out[0] = head_sums(zs[...])
    grad = grad.astype(BF16)
    dr_out[0] = nn(grad, write)
    dw = tn(grad, read)

    @pl.when(b < 2)
    def _():
        dx_out[0] = full[...]
        dw_out[0] = dw

    @pl.when(answer)
    def _():
        adw[0] = dw.astype(BF16)
        for k in range(GROUP):
            there = pl.multiple_of((me[0] ^ k) * ROWS, ROWS)
            outs[k][0] = full[pl.ds(there, ROWS), :]


def token_kernel(me, m2, pw, pd, dxi, dwi, *refs):
    chunks, outs = refs[:GROUP], refs[2 * GROUP : 3 * GROUP]
    pdw, z, closing, ends, full, x = refs[3 * GROUP :]
    gathered(m2, ends)
    assembled(me, chunks, x)
    xs = x[...].astype(F32)
    to_close = closing_weight(pd[0])
    tail = nn(pw[0], ends[...]) * to_close
    full[...] = (dxi[0].astype(F32) + tail).astype(BF16)
    pdw[0] = (dwi[0] + nt((xs * to_close).astype(BF16), ends[...])).astype(BF16)
    tail = tail * xs
    closing[0] = jnp.broadcast_to(jnp.sum(tail, axis=0, keepdims=True), (8, L))
    z[0] = head_sums(tail)
    for k in range(GROUP):
        there = pl.multiple_of((me[0] ^ k) * ROWS, ROWS)
        outs[k][0] = full[pl.ds(there, ROWS), :]


def output_kernel(
    length, m2, m3, pr, pd, pc, ar, ad, ac, yi, dri, zi, z, closing, py, pdr, pdd, ay, adr, add, start, ends
):
    b = pl.program_id(0)
    answer = b == 2
    gathered(m3, start)
    read = jnp.where(answer, ar[0], pr[0])
    decay = jnp.where(answer, ad[0], pd[0])
    alive = jnp.where(answer, length[0], B)
    cot = live_rows(jnp.where(answer, ac[0], pc[0]).astype(F32), alive)
    growth = grown(decay)
    outside = nn(read, start[...]) * growth
    y = yi[0].astype(F32) + outside
    dr = dri[0] + nt((cot * growth).astype(BF16), start[...])
    zs = zi[0] + head_sums(cot * outside) - jnp.where(answer, 0.0, z[0])
    tri = lower()
    dd = sum(nn(part, tri) for part in terms(zs))

    @pl.when(b < 2)
    def _():
        gathered(m2, ends)
        inner = jnp.sum(ends[...].astype(F32) * start[...].astype(F32), axis=0, keepdims=True)
        last = closing[0] + inner * growth[B - 1 : B, :]
        member = (iota((H, L), 1) // HD == iota((H, L), 0)).astype(BF16)
        total = sum(nt(member, part) for part in terms(last))
        py[0] = y.astype(BF16)
        pdr[0] = dr.astype(BF16)
        pdd[0] = dd + total[:, 0:1]

    @pl.when(answer)
    def _():
        ay[0] = live_rows(y, length[0]).astype(BF16)
        adr[0] = dr.astype(BF16)
        add[0] = dd


SMEM = pl.BlockSpec(memory_space=pltpu.SMEM)
VMEM = pl.BlockSpec(memory_space=pltpu.VMEM)
ANY = pl.BlockSpec(memory_space=pl.ANY)


def own(*dims):
    return pl.BlockSpec((1, *dims), lambda b: (jnp.minimum(b, 1), 0, 0))


def one(*dims):
    return pl.BlockSpec((1, *dims), lambda b: (0, 0, 0))


def each(*dims):
    return pl.BlockSpec((1, *dims), lambda b: (b, 0, 0))


def column(width, index):
    return pl.BlockSpec((B, width), lambda b: (0, index(b)))


def shape(dims, dtype=BF16):
    return jax.ShapeDtypeStruct(dims, dtype)


def call(kernel, steps, ins, outs, args, scratch=(), flops=1e9, alias=None, limit=None):
    return pl.pallas_call(
        kernel,
        grid=(steps,),
        in_specs=ins,
        out_specs=[spec for spec, _ in outs],
        out_shape=[struct for _, struct in outs],
        scratch_shapes=scratch,
        input_output_aliases=alias or {},
        compiler_params=pltpu.CompilerParams(vmem_limit_bytes=limit) if limit else None,
        cost_estimate=pl.CostEstimate(flops=int(flops), bytes_accessed=4000000, transcendentals=0),
    )(*args)


def exchange(chunks):
    sent = {0: chunks[0]}
    for offsets in ((4, 5), (2, 3, 6, 7), (1,)):
        for k in offsets:
            sent[k] = lax.ppermute(chunks[k], "head", [(i, i ^ k) for i in range(GROUP)])
    return [sent[k] for k in range(GROUP)]


def transposed(message):
    return lax.all_to_all(message, "seq", split_axis=0, concat_axis=0, tiled=True)


def per_device(pt, pw, pr, pd, pc, at, aw, ar, ad, ac, sizes, length):
    me = lax.axis_index("head").astype(jnp.int32).reshape(1)
    state = pltpu.VMEM((N, L), BF16)
    block = pltpu.VMEM((B, L), BF16)
    chunk = [(each(ROWS, L), shape((3, ROWS, L))) for _ in range(GROUP)]
    pieces = [each(ROWS, L)] * GROUP
    prompt_side = [own(B, N), own(H, B), own(B, L)]
    answer_side = [one(B, N), one(H, B), one(B, L)]
    m1, done = call(
        reach_kernel,
        1,
        [SMEM] + [ANY] * 6,
        [(ANY, shape((B, 3 * HALF + N))), (VMEM, shape((8, N), F32))],
        (length, pr, pd, pc, ar, ad, ac),
        (
            pltpu.VMEM((3, B, N), BF16),
            pltpu.VMEM((3, H, B), F32),
            pltpu.VMEM((3, B, L), BF16),
            pltpu.VMEM((B, 3 * HALF + N), BF16),
            pltpu.VMEM((8, L), F32),
            pltpu.SemaphoreType.DMA((9,)),
            pltpu.SemaphoreType.DMA((4,)),
        ),
    )
    m1 = transposed(m1)
    cut = call(
        split_kernel,
        1,
        [SMEM, ANY, ANY, ANY],
        [(VMEM, shape((3, ROWS, L)))] * GROUP,
        (me, pt, at, done),
        (
            pltpu.SemaphoreType.DMA((2 * GROUP,)),
        ),
        limit=4 << 20,
    )
    cut = exchange(cut)
    m2, factors = call(
        turn_kernel,
        1,
        [SMEM, column(2 * HALF, lambda q: 0), column(HALF, lambda q: 2), column(N, lambda q: 12)],
        [
            (column(2 * HALF, lambda q: 0), shape((B, 4 * HALF))),
            (pl.BlockSpec((2 * SHARDS, HALF), lambda q: (0, 0)), shape((2 * SHARDS, HALF), F32)),
        ],
        (sizes, m1, m1, m1),
        limit=8 << 20,
    )
    (m2,) = call(
        local_kernel,
        2,
        [SMEM, ANY, each(B, N), each(H, B), *pieces],
        [(column(HALF, lambda q: 2 + q), shape((B, 4 * HALF)))],
        (me, m2, pw, pd, *cut),
        (block,),
        alias={1: 0},
        limit=12 << 20,
    )
    m2 = transposed(m2)
    made = call(
        inside_kernel,
        3,
        [SMEM, SMEM, own(B, N), *prompt_side, one(B, N), *answer_side, *pieces],
        [
            *[(pl.BlockSpec((1, ROWS, L), lambda b: (2, 0, 0)), shape((3, ROWS, L)))] * GROUP,
            (each(B, L), shape((3, B, L))),
            (own(B, L), shape((2, B, L))),
            (each(B, N), shape((3, B, N), F32)),
            (own(B, N), shape((2, B, N), F32)),
            (one(B, N), shape((1, B, N))),
            (each(H, B), shape((3, H, B), F32)),
        ],
        (length, me, pw, pr, pd, pc, aw, ar, ad, ac, *cut),
        (block, pltpu.VMEM((B, L), F32), block),
        8e9,
    )
    yi, dxi, dri, dwi, adw, zi = made[GROUP:]
    (m3,) = call(
        start_kernel, 1, [SMEM, VMEM, VMEM], [(VMEM, shape((B, 3 * HALF)))], (sizes, factors, m2), limit=4 << 20
    )
    m3 = transposed(m3)
    made = call(
        token_kernel,
        2,
        [SMEM, column(HALF, lambda q: q), each(B, N), each(H, B), each(B, L), each(B, N), *pieces, *[ANY] * GROUP],
        [
            *chunk,
            (each(B, N), shape((2, B, N))),
            (each(H, B), shape((2, H, B), F32)),
            (each(8, L), shape((2, 8, L), F32)),
        ],
        (me, m2, pw, pd, dxi, dwi, *cut, *made[:GROUP]),
        (state, block, block),
        alias={6 + GROUP + k: k for k in range(GROUP)},
    )
    pdw, z, closing = made[GROUP:]
    back = exchange(made[:GROUP])
    py, pdr, pdd, ay, adr, add = call(
        output_kernel,
        3,
        [
            SMEM,
            column(HALF, lambda b: jnp.minimum(b, 1)),
            column(HALF, lambda b: b),
            *prompt_side,
            *answer_side,
            each(B, L),
            each(B, N),
            each(H, B),
            own(H, B),
            own(8, L),
        ],
        [
            (own(B, L), shape((2, B, L))),
            (own(B, N), shape((2, B, N))),
            (own(H, B), shape((2, H, B), F32)),
            (one(B, L), shape((1, B, L))),
            (one(B, N), shape((1, B, N))),
            (one(H, B), shape((1, H, B), F32)),
        ],
        (length, m2, m3, pr, pd, pc, ar, ad, ac, yi, dri, zi, z, closing),
        (state, state),
    )
    pdx, adx = call(
        join_kernel,
        1,
        [SMEM] + [VMEM] * GROUP,
        [(ANY, shape((2, ROWS, GROUP * L))), (ANY, shape((1, ROWS, GROUP * L)))],
        (me, *back),
        (
            pltpu.SemaphoreType.DMA((2 * GROUP,)),
        ),
        limit=4 << 20,
    )
    return py, pdx, pdw, pdr, pdd, ay, adx, adw, adr, add


def solution(mesh):
    split_positions = P(None, ("seq", "head"), None)
    prompt = P(None, "seq", "head")
    answer = P("seq", None, "head")
    return jax.shard_map(
        per_device,
        mesh=mesh,
        in_specs=(
            split_positions,
            prompt,
            prompt,
            P(None, "head", "seq"),
            prompt,
            P("seq", "head", None),
            answer,
            answer,
            P("seq", "head", None),
            answer,
            P(),
            P("seq"),
        ),
        out_specs=(
            prompt,
            split_positions,
            prompt,
            prompt,
            P(None, "head", "seq"),
            answer,
            P("seq", "head", None),
            answer,
            answer,
            P("seq", "head", None),
        ),
        check_vma=False,
    )
```

```python
import jax
import jax.numpy as jnp
from jax import lax
from jax.experimental import pallas as pl
from jax.experimental.pallas import tpu as pltpu
from jax.sharding import PartitionSpec as P


HD = 64
N = 128
B = 256
H = 16
L = H * HD
SHARDS = 16
GROUP = 8
ROWS = B // GROUP
HALF = L // 2
F32 = jnp.float32
BF16 = jnp.bfloat16


def nn(a, b):
    return lax.dot_general(a, b, (((1,), (0,)), ((), ())), preferred_element_type=F32)


def nt(a, b):
    return lax.dot_general(a, b, (((1,), (1,)), ((), ())), preferred_element_type=F32)


def tn(a, b):
    return lax.dot_general(a, b, (((0,), (0,)), ((), ())), preferred_element_type=F32)


def iota(shape, axis):
    return lax.broadcasted_iota(jnp.int32, shape, axis)


def terms(value):
    high = value.astype(BF16)
    rest = value - high.astype(F32)
    middle = rest.astype(BF16)
    return high, middle, (rest - middle.astype(F32)).astype(BF16)


def upper():
    return (iota((B, B), 0) <= iota((B, B), 1)).astype(BF16)


def lower():
    return (iota((B, B), 1) <= iota((B, B), 0)).astype(BF16)


def running_rows(decay):
    parts = nn(jnp.concatenate([part.astype(F32) for part in terms(decay)], axis=0).astype(BF16), upper())
    return parts[:H] + parts[H : 2 * H] + parts[2 * H :]


def running_columns(decay):
    tri = lower()
    total = None
    for part in terms(decay):
        wide = part.astype(F32)
        added = nt(tri, jnp.concatenate([wide, wide, wide], axis=0).astype(BF16))
        total = added if total is None else total + added
    return total


def widened(columns):
    lane = iota(columns.shape, 1)
    high = columns.astype(BF16).astype(F32)
    rest = columns - high
    middle = rest.astype(BF16).astype(F32)
    packed = jnp.where(lane < H, high, jnp.where(lane < 2 * H, middle, rest - middle)).astype(BF16)
    member = (iota((3 * H, L), 1) // HD == iota((3 * H, L), 0) % H).astype(BF16)
    return nn(packed, member)


def grown(decay):
    return widened(jnp.exp(running_columns(decay)))


def closing_weight(decay):
    columns = running_columns(decay)
    return widened(jnp.exp(columns[B - 1 : B, :] - columns))


def head_sums(values):
    member = (iota((H, L), 1) // HD == iota((H, L), 0)).astype(BF16)
    high = values.astype(BF16)
    low = (values - high.astype(F32)).astype(BF16)
    return nt(member, high) + nt(member, low)


def live_rows(value, length):
    return jnp.where(iota(value.shape, 0) < length, value, jnp.zeros_like(value))


def piece(d):
    return slice(16 * (d // 2), 16 * (d // 2) + 16), slice(HALF * (d % 2), HALF * (d % 2) + HALF)


def scattered(out, state, first):
    for d in range(SHARDS):
        rows, lanes = piece(d)
        out[16 * d : 16 * d + 16, pl.ds(first, HALF)] = state[rows, lanes].astype(BF16)


def gathered(m, place):
    for d in range(SHARDS):
        rows, lanes = piece(d)
        place[rows, lanes] = m[16 * d : 16 * d + 16, :]


def assembled(me, chunks, x):
    for k in range(GROUP):
        there = pl.multiple_of((me[0] ^ k) * ROWS, ROWS)
        x[pl.ds(there, ROWS), :] = chunks[k][0]


def reach_kernel(length, me, pr, pd, pc, ar, ad, ac, out, place, reads, decays, cots, stage, factors, came, went):
    place[0] = me[0]
    coming = []
    for b in range(3):
        group = []
        for i, (prompt, answer, place) in enumerate(((pd, ad, decays), (pr, ar, reads), (pc, ac, cots))):
            source = prompt.at[b] if b < 2 else answer.at[0]
            group.append(pltpu.make_async_copy(source, place.at[b], came.at[3 * b + i]))
            group[-1].start()
        coming.append(group)
    going = []
    for b in range(3):
        for copy in coming[b]:
            copy.wait()
        cot = cots[b].astype(F32)
        if b == 2:
            cot = live_rows(cot, length[0])
        growth = grown(decays[b])
        scattered(stage, tn(reads[b], (cot * growth).astype(BF16)), b * HALF)
        going.append(pltpu.make_async_copy(stage.at[:, pl.ds(b * HALF, HALF)], out.at[:, pl.ds(b * HALF, HALF)], went.at[b]))
        going[-1].start()
        if b < 2:
            last = growth[B - 1 : B, :]
            high = last.astype(BF16).astype(F32)
            factors[2 * b : 2 * b + 1, :] = high
            factors[2 * b + 1 : 2 * b + 2, :] = last - high
        if b == 1:
            for half in range(2):
                lanes = [slice(HALF * half + N * j, HALF * half + N * j + N) for j in range(4)]
                part = jnp.concatenate([factors[i : i + 1, lane] for i in range(4) for lane in lanes], axis=0)
                for d in range(half, SHARDS, 2):
                    stage[16 * d : 16 * d + 16, 3 * HALF :] = part.astype(BF16)
            tail = pl.ds(3 * HALF, N)
            going.append(pltpu.make_async_copy(stage.at[:, tail], out.at[:, tail], went.at[3]))
            going[-1].start()
    for copy in going:
        copy.wait()


def split_kernel(me, pt, at, *refs):
    outs, came = refs[:GROUP], refs[GROUP]
    copies = []
    for k in range(GROUP):
        there = pl.multiple_of((me[0] ^ k) * L, L)
        copies.append(pltpu.make_async_copy(pt.at[:, :, pl.ds(there, L)], outs[k].at[0:2], came.at[2 * k]))
        copies.append(pltpu.make_async_copy(at.at[:, :, pl.ds(there, L)], outs[k].at[2:3], came.at[2 * k + 1]))
    for copy in copies:
        copy.start()
    for copy in copies:
        copy.wait()


def join_kernel(me, *refs):
    ins, (pt, at, went) = refs[:GROUP], refs[GROUP:]
    copies = []
    for k in range(GROUP):
        there = pl.multiple_of((me[0] ^ k) * L, L)
        copies.append(pltpu.make_async_copy(ins[k].at[0:2], pt.at[:, :, pl.ds(there, L)], went.at[2 * k]))
        copies.append(pltpu.make_async_copy(ins[k].at[2:3], at.at[:, :, pl.ds(there, L)], went.at[2 * k + 1]))
    for copy in copies:
        copy.start()
    for copy in copies:
        copy.wait()


def shard_factor(packed, k, q):
    part = packed[16 * k : 16 * k + 16, :].astype(F32)
    rows = [part[8 * q + j : 8 * q + j + 1] + part[8 * q + 4 + j : 8 * q + 5 + j] for j in range(4)]
    return jnp.concatenate(rows, axis=1)


def owner_of(sizes, k):
    return (sizes[0] <= k).astype(jnp.int32) + (sizes[0] + sizes[1] <= k).astype(jnp.int32)


def local_kernel(me, message, pw, pd, *refs):
    chunks, (out, x) = refs[:GROUP], refs[GROUP:]
    assembled(me, chunks, x)
    weighted = (x[...].astype(F32) * closing_weight(pd[0])).astype(BF16)
    scattered(out, tn(pw[0], weighted), 0)


def turn_kernel(sizes, reach, answers, packed, out, factors):
    for q in range(2):
        grad = jnp.zeros((16, HALF), F32)
        for k in range(SHARDS):
            part = answers[16 * k : 16 * k + 16, :].astype(F32)
            grad = grad + part * (owner_of(sizes, k) == q).astype(F32)
        for k in reversed(range(SHARDS)):
            out[16 * k : 16 * k + 16, q * HALF : (q + 1) * HALF] = grad.astype(BF16)
            factor = shard_factor(packed, k, q)
            factors[16 * q + k : 16 * q + k + 1, :] = factor
            grad = reach[16 * k : 16 * k + 16, q * HALF : (q + 1) * HALF].astype(F32) + factor * grad


def start_kernel(sizes, factors, m2, out):
    ends = []
    for q in range(2):
        state = jnp.zeros((16, HALF), F32)
        for k in range(SHARDS):
            out[16 * k : 16 * k + 16, q * HALF : (q + 1) * HALF] = state.astype(BF16)
            local = m2[16 * k : 16 * k + 16, (2 + q) * HALF : (3 + q) * HALF].astype(F32)
            state = factors[16 * q + k : 16 * q + k + 1, :] * state + local
        ends.append(state)
    for k in range(SHARDS):
        owner = owner_of(sizes, k)
        mine = ends[0] * (owner == 0).astype(F32) + ends[1] * (owner == 1).astype(F32)
        out[16 * k : 16 * k + 16, 2 * HALF : 3 * HALF] = mine.astype(BF16)


def inside_kernel(length, me, pw, pr, pd, pc, aw, ar, ad, ac, *refs):
    chunks, outs = refs[:GROUP], refs[GROUP : 2 * GROUP]
    y_out, dx_out, dr_out, dw_out, adw, z_out, x, zs, full = refs[2 * GROUP :]
    b = pl.program_id(0)
    answer = b == 2
    write = jnp.where(answer, aw[0], pw[0])
    read = jnp.where(answer, ar[0], pr[0])
    decay = jnp.where(answer, ad[0], pd[0])
    alive = jnp.where(answer, length[0], B)
    cot32 = live_rows(jnp.where(answer, ac[0], pc[0]).astype(F32), alive)
    cot_t = cot32.T.astype(BF16)
    assembled(me, chunks, x)
    rows = running_rows(decay)
    columns = running_columns(decay)
    scores = nt(read, write)
    causal = iota((B, B), 0) >= iota((B, B), 1)
    first = iota((B, 2 * HD), 1) < HD
    grad = jnp.zeros((B, B), F32)
    for pair in range(H // 2):
        lanes = slice(2 * HD * pair, 2 * HD * pair + 2 * HD)
        xs = x[:, lanes]
        cs = cot32[:, lanes]
        ys, dxs = [], []
        for s in range(2):
            h = 2 * pair + s
            gap = columns[:, h : h + 1] - rows[h : h + 1, :]
            weight = jnp.exp(jnp.where(causal, gap, -1e30))
            mixing = (weight * scores).astype(BF16)
            ys.append(nn(mixing, xs))
            dxs.append(nn(cot_t[HD * h : HD * h + HD, :], mixing))
            own = jnp.where(first if s == 0 else jnp.logical_not(first), cs, 0.0).astype(BF16)
            grad = grad + nt(own, xs) * weight
        y = jnp.where(first, ys[0], ys[1])
        dx = jnp.concatenate(dxs, axis=0).T
        y_out[0, :, lanes] = y.astype(BF16)
        full[:, lanes] = dx.astype(BF16)
        zs[:, lanes] = cs * y - xs.astype(F32) * dx
    z_out[0] = head_sums(zs[...])
    grad = grad.astype(BF16)
    dr_out[0] = nn(grad, write)
    dw = tn(grad, read)

    @pl.when(b < 2)
    def _():
        dx_out[0] = full[...]
        dw_out[0] = dw

    @pl.when(answer)
    def _():
        adw[0] = dw.astype(BF16)
        for k in range(GROUP):
            there = pl.multiple_of((me[0] ^ k) * ROWS, ROWS)
            outs[k][0] = full[pl.ds(there, ROWS), :]


def token_kernel(me, m2, pw, pd, dxi, dwi, *refs):
    chunks, outs = refs[:GROUP], refs[2 * GROUP : 3 * GROUP]
    pdw, z, closing, ends, full, x = refs[3 * GROUP :]
    gathered(m2, ends)
    assembled(me, chunks, x)
    xs = x[...].astype(F32)
    to_close = closing_weight(pd[0])
    tail = nn(pw[0], ends[...]) * to_close
    full[...] = (dxi[0].astype(F32) + tail).astype(BF16)
    pdw[0] = (dwi[0] + nt((xs * to_close).astype(BF16), ends[...])).astype(BF16)
    tail = tail * xs
    closing[0] = jnp.broadcast_to(jnp.sum(tail, axis=0, keepdims=True), (8, L))
    z[0] = head_sums(tail)
    for k in range(GROUP):
        there = pl.multiple_of((me[0] ^ k) * ROWS, ROWS)
        outs[k][0] = full[pl.ds(there, ROWS), :]


def output_kernel(
    length, m2, m3, pr, pd, pc, ar, ad, ac, yi, dri, zi, z, closing, py, pdr, pdd, ay, adr, add, start, ends
):
    b = pl.program_id(0)
    answer = b == 2
    gathered(m3, start)
    read = jnp.where(answer, ar[0], pr[0])
    decay = jnp.where(answer, ad[0], pd[0])
    alive = jnp.where(answer, length[0], B)
    cot = live_rows(jnp.where(answer, ac[0], pc[0]).astype(F32), alive)
    growth = grown(decay)
    outside = nn(read, start[...]) * growth
    y = yi[0].astype(F32) + outside
    dr = dri[0] + nt((cot * growth).astype(BF16), start[...])
    zs = zi[0] + head_sums(cot * outside) - jnp.where(answer, 0.0, z[0])
    tri = lower()
    dd = sum(nn(part, tri) for part in terms(zs))

    @pl.when(b < 2)
    def _():
        gathered(m2, ends)
        inner = jnp.sum(ends[...].astype(F32) * start[...].astype(F32), axis=0, keepdims=True)
        last = closing[0] + inner * growth[B - 1 : B, :]
        member = (iota((H, L), 1) // HD == iota((H, L), 0)).astype(BF16)
        total = sum(nt(member, part) for part in terms(last))
        py[0] = y.astype(BF16)
        pdr[0] = dr.astype(BF16)
        pdd[0] = dd + total[:, 0:1]

    @pl.when(answer)
    def _():
        ay[0] = live_rows(y, length[0]).astype(BF16)
        adr[0] = dr.astype(BF16)
        add[0] = dd


SMEM = pl.BlockSpec(memory_space=pltpu.SMEM)
VMEM = pl.BlockSpec(memory_space=pltpu.VMEM)
ANY = pl.BlockSpec(memory_space=pl.ANY)


def own(*dims):
    return pl.BlockSpec((1, *dims), lambda b: (jnp.minimum(b, 1), 0, 0))


def one(*dims):
    return pl.BlockSpec((1, *dims), lambda b: (0, 0, 0))


def each(*dims):
    return pl.BlockSpec((1, *dims), lambda b: (b, 0, 0))


def column(width, index):
    return pl.BlockSpec((B, width), lambda b: (0, index(b)))


def shape(dims, dtype=BF16):
    return jax.ShapeDtypeStruct(dims, dtype)


def call(kernel, steps, ins, outs, args, scratch=(), flops=1e9, alias=None, limit=None):
    return pl.pallas_call(
        kernel,
        grid=(steps,),
        in_specs=ins,
        out_specs=[spec for spec, _ in outs],
        out_shape=[struct for _, struct in outs],
        scratch_shapes=scratch,
        input_output_aliases=alias or {},
        compiler_params=pltpu.CompilerParams(vmem_limit_bytes=limit) if limit else None,
        cost_estimate=pl.CostEstimate(flops=int(flops), bytes_accessed=4000000, transcendentals=0),
    )(*args)


def exchange(chunks):
    sent = {0: chunks[0]}
    for offsets in ((4, 5), (2, 3, 6, 7), (1,)):
        for k in offsets:
            sent[k] = lax.ppermute(chunks[k], "head", [(i, i ^ k) for i in range(GROUP)])
    return [sent[k] for k in range(GROUP)]


def transposed(message):
    return lax.all_to_all(message, "seq", split_axis=0, concat_axis=0, tiled=True)


def per_device(pt, pw, pr, pd, pc, at, aw, ar, ad, ac, sizes, length):
    me = lax.axis_index("head").astype(jnp.int32).reshape(1)
    state = pltpu.VMEM((N, L), BF16)
    block = pltpu.VMEM((B, L), BF16)
    chunk = [(each(ROWS, L), shape((3, ROWS, L))) for _ in range(GROUP)]
    pieces = [each(ROWS, L)] * GROUP
    prompt_side = [own(B, N), own(H, B), own(B, L)]
    answer_side = [one(B, N), one(H, B), one(B, L)]
    m1, place = call(
        reach_kernel,
        1,
        [SMEM, SMEM] + [ANY] * 6,
        [(ANY, shape((B, 3 * HALF + N))), (SMEM, shape((1,), jnp.int32))],
        (length, me, pr, pd, pc, ar, ad, ac),
        (
            pltpu.VMEM((3, B, N), BF16),
            pltpu.VMEM((3, H, B), F32),
            pltpu.VMEM((3, B, L), BF16),
            pltpu.VMEM((B, 3 * HALF + N), BF16),
            pltpu.VMEM((8, L), F32),
            pltpu.SemaphoreType.DMA((9,)),
            pltpu.SemaphoreType.DMA((4,)),
        ),
    )
    m1 = transposed(m1)
    cut = call(
        split_kernel,
        1,
        [SMEM, ANY, ANY],
        [(VMEM, shape((3, ROWS, L)))] * GROUP,
        (place, pt, at),
        (
            pltpu.SemaphoreType.DMA((2 * GROUP,)),
        ),
        limit=4 << 20,
    )
    cut = exchange(cut)
    m2, factors = call(
        turn_kernel,
        1,
        [SMEM, column(2 * HALF, lambda q: 0), column(HALF, lambda q: 2), column(N, lambda q: 12)],
        [
            (column(2 * HALF, lambda q: 0), shape((B, 4 * HALF))),
            (pl.BlockSpec((2 * SHARDS, HALF), lambda q: (0, 0)), shape((2 * SHARDS, HALF), F32)),
        ],
        (sizes, m1, m1, m1),
        limit=8 << 20,
    )
    (m2,) = call(
        local_kernel,
        2,
        [SMEM, ANY, each(B, N), each(H, B), *pieces],
        [(column(HALF, lambda q: 2 + q), shape((B, 4 * HALF)))],
        (me, m2, pw, pd, *cut),
        (block,),
        alias={1: 0},
        limit=12 << 20,
    )
    m2 = transposed(m2)
    made = call(
        inside_kernel,
        3,
        [SMEM, SMEM, own(B, N), *prompt_side, one(B, N), *answer_side, *pieces],
        [
            *[(pl.BlockSpec((1, ROWS, L), lambda b: (2, 0, 0)), shape((3, ROWS, L)))] * GROUP,
            (each(B, L), shape((3, B, L))),
            (own(B, L), shape((2, B, L))),
            (each(B, N), shape((3, B, N), F32)),
            (own(B, N), shape((2, B, N), F32)),
            (one(B, N), shape((1, B, N))),
            (each(H, B), shape((3, H, B), F32)),
        ],
        (length, me, pw, pr, pd, pc, aw, ar, ad, ac, *cut),
        (block, pltpu.VMEM((B, L), F32), block),
        8e9,
    )
    yi, dxi, dri, dwi, adw, zi = made[GROUP:]
    (m3,) = call(
        start_kernel, 1, [SMEM, VMEM, VMEM], [(VMEM, shape((B, 3 * HALF)))], (sizes, factors, m2), limit=4 << 20
    )
    m3 = transposed(m3)
    made = call(
        token_kernel,
        2,
        [SMEM, column(HALF, lambda q: q), each(B, N), each(H, B), each(B, L), each(B, N), *pieces, *[ANY] * GROUP],
        [
            *chunk,
            (each(B, N), shape((2, B, N))),
            (each(H, B), shape((2, H, B), F32)),
            (each(8, L), shape((2, 8, L), F32)),
        ],
        (me, m2, pw, pd, dxi, dwi, *cut, *made[:GROUP]),
        (state, block, block),
        alias={6 + GROUP + k: k for k in range(GROUP)},
    )
    pdw, z, closing = made[GROUP:]
    back = exchange(made[:GROUP])
    py, pdr, pdd, ay, adr, add = call(
        output_kernel,
        3,
        [
            SMEM,
            column(HALF, lambda b: jnp.minimum(b, 1)),
            column(HALF, lambda b: b),
            *prompt_side,
            *answer_side,
            each(B, L),
            each(B, N),
            each(H, B),
            own(H, B),
            own(8, L),
        ],
        [
            (own(B, L), shape((2, B, L))),
            (own(B, N), shape((2, B, N))),
            (own(H, B), shape((2, H, B), F32)),
            (one(B, L), shape((1, B, L))),
            (one(B, N), shape((1, B, N))),
            (one(H, B), shape((1, H, B), F32)),
        ],
        (length, m2, m3, pr, pd, pc, ar, ad, ac, yi, dri, zi, z, closing),
        (state, state),
    )
    pdx, adx = call(
        join_kernel,
        1,
        [SMEM] + [VMEM] * GROUP,
        [(ANY, shape((2, ROWS, GROUP * L))), (ANY, shape((1, ROWS, GROUP * L)))],
        (me, *back),
        (
            pltpu.SemaphoreType.DMA((2 * GROUP,)),
        ),
        limit=4 << 20,
    )
    return py, pdx, pdw, pdr, pdd, ay, adx, adw, adr, add


def solution(mesh):
    split_positions = P(None, ("seq", "head"), None)
    prompt = P(None, "seq", "head")
    answer = P("seq", None, "head")
    return jax.shard_map(
        per_device,
        mesh=mesh,
        in_specs=(
            split_positions,
            prompt,
            prompt,
            P(None, "head", "seq"),
            prompt,
            P("seq", "head", None),
            answer,
            answer,
            P("seq", "head", None),
            answer,
            P(),
            P("seq"),
        ),
        out_specs=(
            prompt,
            split_positions,
            prompt,
            prompt,
            P(None, "head", "seq"),
            answer,
            P("seq", "head", None),
            answer,
            answer,
            P("seq", "head", None),
        ),
        check_vma=False,
    )
```
